16 devices in a mesh: data: 16 (over z, y, x, core).
Axes of the slice: x: 2, y: 2, z: 2, core: 2. Of those that a mesh axis runs over, the one named last changes fastest.
Arguments:
- tokens: bfloat16 [8192, 1024], P('data')
- labels: int32 [2, 8192], P(None, 'data')
- w_one: bfloat16 [1024, 4096], replicated
- w_two: bfloat16 [4096, 1024], replicated
- adapter_a: bfloat16 [1024, 16], replicated
- adapter_b: bfloat16 [16, 4096], replicated
- task_heads: bfloat16 [2, 1024, 19], replicated
Outputs:
- output 1: float32 [2], replicated
- output 2: float32 [1024, 16], P('data')
- output 3: float32 [16, 4096], P(None, 'data')
All inputs are finite; a program needn't handle non-finite values.
Results may differ from the reference program's by a relative error of at most 0.00221719.
Values are sent between devices in bfloat16 or wider.
A program may use at most 1 GiB of HBM per device.

```python
import jax
import jax.numpy as jnp
from jax import lax

DEVICES = 16
TOK_DEV = 512
D_MODEL = 1024
D_FF = 4096
LORA_RANK = 16
NUM_TASKS = 2
NUM_CLASSES = 19
EG_STEPS = 20


def draw_labels(label_key):
    key_list = jax.random.split(label_key, 4)
    total_tok = DEVICES * TOK_DEV
    dev_shift = jax.random.randint(key_list[0], (DEVICES, 1), 0, NUM_CLASSES)
    half_width = (NUM_CLASSES + 1) // 2
    common_lab = (dev_shift + jax.random.randint(key_list[1], (DEVICES, TOK_DEV), 0, half_width)) % NUM_CLASSES
    common_lab = common_lab.reshape(total_tok)
    own_lab = jax.random.randint(key_list[2], (NUM_TASKS, total_tok), 0, NUM_CLASSES)
    pick_common = jax.random.randint(key_list[3], (NUM_TASKS, total_tok), 0, 5) < 3
    return jnp.where(pick_common, common_lab[None, :], own_lab).astype(jnp.int32)


def setup_inputs(seed: int = 0) -> dict:
    key_list = jax.random.split(jax.random.key(seed), 8)
    total_tok = DEVICES * TOK_DEV
    tokens = jax.random.normal(key_list[0], (total_tok, D_MODEL), jnp.float32)
    w_one = jax.random.normal(key_list[1], (D_MODEL, D_FF), jnp.float32) * D_MODEL ** -0.5
    w_two = jax.random.normal(key_list[2], (D_FF, D_MODEL), jnp.float32) * D_FF ** -0.5
    adapter_a = jax.random.normal(key_list[3], (D_MODEL, LORA_RANK), jnp.float32) * D_MODEL ** -0.5
    adapter_b = jax.random.normal(key_list[4], (LORA_RANK, D_FF), jnp.float32) * LORA_RANK ** -0.5
    head_common = jax.random.normal(key_list[5], (D_MODEL, NUM_CLASSES), jnp.float32)
    head_own = jax.random.normal(key_list[6], (NUM_TASKS, D_MODEL, NUM_CLASSES), jnp.float32)
    head_sign = jnp.where(jnp.arange(NUM_TASKS) % 2 == 0, 1.0, -1.0)
    task_heads = (head_sign[:, None, None] * head_common[None] + 0.8 * head_own) * (1.5 * D_MODEL ** -0.5)
    labels = draw_labels(key_list[7])
    return {
        "tokens": tokens.astype(jnp.bfloat16),
        "labels": labels,
        "w_one": w_one.astype(jnp.bfloat16),
        "w_two": w_two.astype(jnp.bfloat16),
        "adapter_a": adapter_a.astype(jnp.bfloat16),
        "adapter_b": adapter_b.astype(jnp.bfloat16),
        "task_heads": task_heads.astype(jnp.bfloat16),
    }


def block_grads(tok_blk, lab_blk, w_one, w_two, adapter_a, adapter_b, task_heads):
    low_rank = jnp.dot(tok_blk, adapter_a, preferred_element_type=jnp.float32).astype(jnp.bfloat16)
    pre_act = jnp.dot(tok_blk, w_one, preferred_element_type=jnp.float32) + jnp.dot(low_rank, adapter_b, preferred_element_type=jnp.float32)
    gelu_out, gelu_slope = jax.jvp(jax.nn.gelu, (pre_act,), (jnp.ones_like(pre_act),))
    hidden = gelu_out.astype(jnp.bfloat16)
    trunk_out = (tok_blk.astype(jnp.float32) + jnp.dot(hidden, w_two, preferred_element_type=jnp.float32)).astype(jnp.bfloat16)
    logits = jnp.einsum("bd,tdc->tbc", trunk_out.astype(jnp.float32), task_heads.astype(jnp.float32))
    task_probs = jax.nn.softmax(logits, axis=-1)
    onehot = (lab_blk[:, :, None] == jnp.arange(NUM_CLASSES)[None, None, :]).astype(jnp.float32)
    logit_err = (task_probs - onehot).astype(jnp.bfloat16)
    d_trunk = jnp.einsum("tbc,tdc->tbd", logit_err.astype(jnp.float32), task_heads.astype(jnp.float32)).astype(jnp.bfloat16)
    d_hidden = jnp.einsum("tbd,fd->tbf", d_trunk.astype(jnp.float32), w_two.astype(jnp.float32))
    d_pre = (d_hidden * gelu_slope[None]).astype(jnp.bfloat16)
    part_b = jnp.einsum("br,tbf->trf", low_rank.astype(jnp.float32), d_pre.astype(jnp.float32))
    d_low = jnp.einsum("tbf,rf->tbr", d_pre.astype(jnp.float32), adapter_b.astype(jnp.float32)).astype(jnp.bfloat16)
    part_a = jnp.einsum("bd,tbr->tdr", tok_blk.astype(jnp.float32), d_low.astype(jnp.float32))
    return part_a, part_b


def reference(tokens, labels, w_one, w_two, adapter_a, adapter_b, task_heads):
    tok_blocks = tokens.reshape(DEVICES, TOK_DEV, D_MODEL)
    lab_blocks = labels.reshape(NUM_TASKS, DEVICES, TOK_DEV).transpose(1, 0, 2)

    def add_block(run_sum, block_in):
        part_a, part_b = block_grads(block_in[0], block_in[1], w_one, w_two, adapter_a, adapter_b, task_heads)
        return (run_sum[0] + part_a, run_sum[1] + part_b), None

    zero_init = (jnp.zeros((NUM_TASKS, D_MODEL, LORA_RANK), jnp.float32), jnp.zeros((NUM_TASKS, LORA_RANK, D_FF), jnp.float32))
    sums, _ = lax.scan(add_block, zero_init, (tok_blocks, lab_blocks))
    batch_total = DEVICES * TOK_DEV
    grad_a = sums[0] / batch_total
    grad_b = sums[1] / batch_total
    gram_mat = jnp.einsum("tdr,sdr->ts", grad_a, grad_a) + jnp.einsum("trf,srf->ts", grad_b, grad_b)
    eg_scale = jnp.trace(gram_mat) / NUM_TASKS

    def eg_step(weights, _):
        weights = weights * jnp.exp(-jnp.sum(gram_mat * weights[None, :], axis=1) / eg_scale)
        return weights / jnp.sum(weights), None

    task_weights, _ = lax.scan(eg_step, jnp.full((NUM_TASKS,), 1.0 / NUM_TASKS, jnp.float32), None, length=EG_STEPS)
    comb_a = jnp.sum(task_weights[:, None, None] * grad_a, axis=0)
    comb_b = jnp.sum(task_weights[:, None, None] * grad_b, axis=0)
    return (task_weights, comb_a, comb_b)
```

```python
import functools

import jax
import jax.numpy as jnp
from jax import lax
from jax.experimental import pallas as pl
from jax.experimental.pallas import tpu as pltpu
from jax.sharding import PartitionSpec as P

EG_STEPS = 20
BF = jnp.bfloat16
F32 = jnp.float32
GELU_C = 0.7978845608028654
GELU_A = 0.044715
MESH = pl.DeviceIdType.MESH
BITS = (1, 2, 4, 8)
NT = (((1,), (1,)), ((), ()))
TN = (((0,), (0,)), ((), ()))


def xor(a, b):
    return sum(bit * ((a // bit + b // bit) % 2) for bit in BITS)


def mm(a, b, dims=(((1,), (0,)), ((), ()))):
    return lax.dot_general(a, b, dims, preferred_element_type=F32)


def kernel(cfg, x_hbm, lab_hbm, w1_hbm, w2_hbm, a_hbm, b_hbm, head_hbm, alpha_ref, ga_ref, gb_ref, xu, w1b, w2, a_v, head_v, lab_v, head_t, u_t, p0, p1, act, slope, z, dz, dp0, dp1, du_t, send_b, recv_b, send_a, recv_a, send_m, recv_m, load_sem, sb_sem, rb_sem, sa_sem, ra_sem, sm_sem, rm_sem):
    n_dev, total = cfg
    tok, d_model = x_hbm.shape
    d_ff = w1_hbm.shape[1]
    rank = a_hbm.shape[0]
    n_cls = head_hbm.shape[0]
    col = d_ff // n_dev
    fc = 2 * col
    n_ch = n_dev // 2
    zc = d_model // 4
    me = lax.axis_index("data")
    chip, core = me // 2, me % 2

    barrier = pltpu.get_barrier_semaphore()
    for k in range(1, n_dev):
        pl.semaphore_signal(barrier, inc=1, device_id=(xor(me, k),), device_id_type=MESH)

    def w1_load(i):
        cols = pl.ds(pl.multiple_of(i * fc, fc), fc)
        return pltpu.make_async_copy(w1_hbm.at[:, cols], w1b.at[pl.ds(0, d_model), cols], load_sem.at[i])

    def w2_load(i):
        cols = pl.ds(pl.multiple_of(i * zc, zc), zc)
        return pltpu.make_async_copy(w2_hbm.at[:, cols], w2.at[:, cols], load_sem.at[n_ch + i])

    base = n_ch + 4
    load_x = pltpu.make_async_copy(x_hbm, xu.at[:, pl.ds(0, d_model)], load_sem.at[base])
    load_a = pltpu.make_async_copy(a_hbm, a_v, load_sem.at[base + 1])
    load_b = pltpu.make_async_copy(b_hbm, w1b.at[pl.ds(d_model, rank), :], load_sem.at[base + 2])
    load_h = pltpu.make_async_copy(head_hbm, head_v, load_sem.at[base + 3])
    load_l = pltpu.make_async_copy(lab_hbm, lab_v, load_sem.at[base + 4])
    load_x.start()
    load_a.start()
    w1_load(0).start()
    load_b.start()
    w1_load(1).start()
    load_h.start()
    load_l.start()
    for i in range(2, n_ch):
        w1_load(i).start()
    for i in range(4):
        w2_load(i).start()

    pad = xu.shape[1] - d_model
    xu[:, d_model:] = jnp.zeros((tok, pad), BF)
    w1b[d_model + rank:, :] = jnp.zeros((pad - rank, d_ff), BF)
    du_t[...] = jnp.zeros_like(du_t)
    load_x.wait()
    load_a.wait()
    low = mm(xu[:, :d_model], a_v[...], NT)
    xu[:, d_model:d_model + rank] = low.astype(BF)
    u_t[...] = low.T.astype(BF)

    def pre(i, p_ref):
        w1_load(i).wait()
        p_ref[...] = mm(xu[...], w1b[:, pl.ds(pl.multiple_of(i * fc, fc), fc)])

    def gelu(i, p_ref):
        x = p_ref[...]
        x2 = x * x
        t = jnp.tanh(x * (GELU_C + (GELU_C * GELU_A) * x2))
        hx = 0.5 * x
        t1 = 1.0 + t
        act[:, pl.ds(pl.multiple_of(i * fc, fc), fc)] = (hx * t1).astype(BF)
        slope[i] = 0.5 * t1 + (hx * (1.0 - t * t)) * (GELU_C + (3.0 * GELU_C * GELU_A) * x2)

    load_b.wait()
    pre(0, p0)

    def fwd(j, _):
        pre(2 * j + 1, p1)
        gelu(2 * j, p0)
        pre(2 * j + 2, p0)
        gelu(2 * j + 1, p1)
        return 0

    lax.fori_loop(0, n_ch // 2 - 1, fwd, 0)
    pre(n_ch - 1, p1)
    gelu(n_ch - 2, p0)

    load_h.wait()
    load_l.wait()
    head_t[...] = jnp.zeros_like(head_t)
    for t in range(2):
        head_t[32 * t:32 * t + n_cls, :] = head_v[:, t, :]
    gelu(n_ch - 1, p1)

    def out_block(i, _):
        w2_load(i).wait()
        cols = pl.ds(pl.multiple_of(i * zc, zc), zc)
        z[:, cols] = (xu[:, cols].astype(F32) + mm(act[...], w2[:, cols])).astype(BF)
        return 0

    lax.fori_loop(0, 4, out_block, 0)

    logits = mm(head_t[...], z[...], NT)
    rows = lax.broadcasted_iota(jnp.int32, (32, tok), 0)
    for t in range(2):
        lg = jnp.where(rows < n_cls, logits[32 * t:32 * t + 32], -jnp.inf)
        ex = jnp.exp(lg - jnp.max(lg, axis=0, keepdims=True))
        prob = ex / jnp.sum(ex, axis=0, keepdims=True)
        err = (prob - (rows == lab_v[t:t + 1, :]).astype(F32)).astype(BF)
        dz[tok * t:tok * t + tok, :] = mm(err, head_t[32 * t:32 * t + 32, :], TN).astype(BF)

    pl.semaphore_wait(barrier, n_dev - 1)

    def chunk_of(kk):
        return xor(chip, kk)

    def d_pre(kk, dp_ref):
        c = chunk_of(kk)
        dh = mm(dz[...], w2[pl.ds(pl.multiple_of(c * fc, fc), fc), :], NT)
        sl = slope[c]
        for t in range(2):
            dp_ref[tok * t:tok * t + tok, :] = (dh[tok * t:tok * t + tok] * sl).astype(BF)

    def b_copy(kk, half):
        dst_core = half
        k = 2 * kk + (core + half) % 2
        return pltpu.make_async_remote_copy(
            src_ref=send_b.at[kk, half], dst_ref=recv_b.at[k], send_sem=sb_sem.at[k], recv_sem=rb_sem.at[k],
            device_id=(2 * chunk_of(kk) + dst_core,), device_id_type=MESH)

    def grads(kk, dp_ref):
        c = chunk_of(kk)
        for t in range(2):
            gb = mm(u_t[...], dp_ref[tok * t:tok * t + tok, :])
            for half in range(2):
                send_b[kk, half, t] = gb[:, col * half:col * half + col]
        bm = w1b[pl.ds(d_model, rank), pl.ds(pl.multiple_of(c * fc, fc), fc)]
        du_t[...] += mm(bm, dp_ref[...], NT)

    d_pre(n_ch - 1, dp0)

    def bwd(j, _):
        kk = n_ch - 1 - 2 * j
        d_pre(kk - 1, dp1)
        grads(kk, dp0)
        b_copy(kk, 0).start()
        b_copy(kk, 1).start()
        d_pre(kk - 2, dp0)
        grads(kk - 1, dp1)
        b_copy(kk - 1, 0).start()
        b_copy(kk - 1, 1).start()
        return 0

    lax.fori_loop(0, n_ch // 2 - 1, bwd, 0)
    d_pre(0, dp1)
    grads(1, dp0)
    b_copy(1, 0).start()
    b_copy(1, 1).start()
    grads(0, dp1)
    b_copy(0, 1 - core).start()

    lane = lax.broadcasted_iota(jnp.int32, (rank, 128), 1)
    ga = [mm(du_t[:, tok * t:tok * t + tok].astype(BF), xu[:, :d_model]) for t in range(2)]
    for j in range(n_ch):
        a0, a1 = (ga[t][:, 128 * j:128 * j + 128] for t in range(2))
        send_a[2 * j] = jnp.where(lane < 64, a0, pltpu.roll(a1, 64, 1))
        send_a[2 * j + 1] = jnp.where(lane < 64, pltpu.roll(a0, 64, 1), a1)

    def a_copy(k):
        dst = xor(me, k)
        return pltpu.make_async_remote_copy(
            src_ref=send_a.at[dst], dst_ref=recv_a.at[k], send_sem=sa_sem.at[k], recv_sem=ra_sem.at[k],
            device_id=(dst,), device_id_type=MESH)

    def m_copy(k):
        return pltpu.make_async_remote_copy(
            src_ref=send_m, dst_ref=recv_m.at[k], send_sem=sm_sem.at[k], recv_sem=rm_sem.at[k],
            device_id=(xor(me, k),), device_id_type=MESH)

    order = [15, 14, 13, 11, 10, 7, 6, 12, 9, 5, 3, 8, 4, 2, 1]
    for k in order:
        a_copy(k).start()

    def b_half(k):
        return b_copy(k // 2, (core + k) % 2)

    sum_b = send_b[0, core]
    for k in reversed(range(1, n_dev)):
        b_half(k).wait_recv()
        sum_b = sum_b + recv_b[k]
    sum_b = sum_b * (1.0 / total)
    b0, b1 = sum_b[0], sum_b[1]
    sq0, sq1, cross = b0 * b0, b1 * b1, b0 * b1
    sum_a = send_a[me]
    for k in reversed(order):
        a_copy(k).wait_recv()
        sum_a = sum_a + recv_a[k]
    sum_a = sum_a * (1.0 / total)
    sq = sum_a * sum_a
    sign = jnp.where(lane < 64, 1.0, -1.0)
    other = pltpu.roll(sum_a, 64, 1)

    def fold(part_b, part_a):
        return jnp.sum(part_b[:, :128] + part_b[:, 128:] + part_a, axis=0, keepdims=True)

    diff = fold(sq0 - sq1, sq * sign)
    both = fold(sq0 + sq1, sq)
    mix = fold(cross, 0.5 * sum_a * other)
    send_m[0:1, :] = diff
    send_m[1:2, :] = both
    send_m[2:3, :] = mix
    send_m[3:4, :] = jnp.zeros_like(mix)
    for k in order:
        m_copy(k).start()
    sum_m = send_m[...]
    for k in reversed(order):
        m_copy(k).wait_recv()
        sum_m = sum_m + recv_m[k]
    gram = jnp.broadcast_to(jnp.sum(sum_m, axis=1, keepdims=True), sum_m.shape)
    m_diff, m_both, m_mix = gram[0:1], gram[1:2], gram[2:3]
    scale = 0.5 / m_both
    c0 = m_diff * scale
    c1 = (m_both - 2.0 * m_mix) * scale
    e = jnp.zeros_like(c0)
    for _ in range(EG_STEPS):
        e = e - (c0 + c1 * jnp.tanh(e))
    al0 = 1.0 / (1.0 + jnp.exp(-2.0 * e))
    al1 = 1.0 / (1.0 + jnp.exp(2.0 * e))
    gb_ref[...] = al0[:, 0:1] * b0 + al1[:, 0:1] * b1
    ga_ref[...] = (al0 * sum_a + al1 * other)[:, :64]
    alpha_ref[...] = jnp.where(lane[0:1, :] == 0, al0, al1)[:, 0:2]
    for k in range(1, n_dev):
        b_half(k).wait_send()
        a_copy(k).wait_send()
        m_copy(k).wait_send()


def solution(mesh):
    n_dev = mesh.shape["data"]

    def device_step(tokens, labels, w_one, w_two, adapter_a, adapter_b, task_heads):
        tok, d_model = tokens.shape
        d_ff = w_one.shape[1]
        rank = adapter_a.shape[1]
        n_tasks, _, n_cls = task_heads.shape
        col = d_ff // n_dev
        fc = 2 * col
        dma = pltpu.SemaphoreType.DMA
        alpha, ga, gb = pl.pallas_call(
            functools.partial(kernel, (n_dev, tok * n_dev)),
            out_shape=(
                jax.ShapeDtypeStruct((1, n_tasks), F32),
                jax.ShapeDtypeStruct((rank, d_model // n_dev), F32),
                jax.ShapeDtypeStruct((rank, col), F32),
            ),
            in_specs=[pl.BlockSpec(memory_space=pl.ANY)] * 7,
            out_specs=[pl.BlockSpec(memory_space=pltpu.VMEM)] * 3,
            scratch_shapes=[
                pltpu.VMEM((tok, d_model + 128), BF),
                pltpu.VMEM((d_model + 128, d_ff), BF),
                pltpu.VMEM((d_ff, d_model), BF),
                pltpu.VMEM((rank, d_model), BF),
                pltpu.VMEM((n_cls, n_tasks, d_model), BF),
                pltpu.VMEM((n_tasks, tok), jnp.int32),
                pltpu.VMEM((n_tasks * 32, d_model), BF),
                pltpu.VMEM((rank, tok), BF),
                pltpu.VMEM((tok, fc), F32),
                pltpu.VMEM((tok, fc), F32),
                pltpu.VMEM((tok, d_ff), BF),
                pltpu.VMEM((n_dev // 2, tok, fc), F32),
                pltpu.VMEM((tok, d_model), BF),
                pltpu.VMEM((n_tasks * tok, d_model), BF),
                pltpu.VMEM((n_tasks * tok, fc), BF),
                pltpu.VMEM((n_tasks * tok, fc), BF),
                pltpu.VMEM((rank, n_tasks * tok), F32),
                pltpu.VMEM((n_dev // 2, 2, n_tasks, rank, col), F32),
                pltpu.VMEM((n_dev, n_tasks, rank, col), F32),
                pltpu.VMEM((n_dev, rank, 128), F32),
                pltpu.VMEM((n_dev, rank, 128), F32),
                pltpu.VMEM((4, 128), F32),
                pltpu.VMEM((n_dev, 4, 128), F32),
                dma((n_dev // 2 + 9,)),
                dma((n_dev,)), dma((n_dev,)), dma((n_dev,)), dma((n_dev,)), dma((n_dev,)), dma((n_dev,)),
            ],
            compiler_params=pltpu.CompilerParams(collective_id=0, has_side_effects=True, vmem_limit_bytes=60 * 1024 * 1024),
            name="step",
        )(tokens, labels, w_one, w_two, adapter_a.T, adapter_b, task_heads.transpose(2, 0, 1))
        return alpha.reshape(n_tasks), ga.T, gb

    return jax.shard_map(device_step, mesh=mesh, in_specs=(P("data", None), P(None, "data"), P(), P(), P(), P(), P()), out_specs=(P(), P("data", None), P(None, "data")), check_vma=False)
```

```python
import functools

import jax
import jax.numpy as jnp
from jax import lax
from jax.experimental import pallas as pl
from jax.experimental.pallas import tpu as pltpu
from jax.sharding import PartitionSpec as P

EG_STEPS = 20
BF = jnp.bfloat16
F32 = jnp.float32
GELU_C = 0.7978845608028654
GELU_A = 0.044715
MESH = pl.DeviceIdType.MESH
BITS = (1, 2, 4, 8)
NT = (((1,), (1,)), ((), ()))
TN = (((0,), (0,)), ((), ()))


def xor(a, b):
    return sum(bit * ((a // bit + b // bit) % 2) for bit in BITS)


def mm(a, b, dims=(((1,), (0,)), ((), ()))):
    return lax.dot_general(a, b, dims, preferred_element_type=F32)


def kernel(cfg, x_hbm, lab_hbm, w1_hbm, w2_hbm, a_hbm, b_hbm, head_hbm, alpha_ref, ga_ref, gb_ref, xu, w1b, w2, a_v, head_v, lab_v, head_t, u_t, p0, p1, act, slope, z, dz, dp0, dp1, du_t, send_b, recv_b, send_a, recv_a, send_m, recv_m, load_sem, sb_sem, rb_sem, sa_sem, ra_sem, sm_sem, rm_sem):
    n_dev, total = cfg
    tok, d_model = x_hbm.shape
    d_ff = w1_hbm.shape[1]
    rank = a_hbm.shape[0]
    n_cls = head_hbm.shape[0]
    col = d_ff // n_dev
    fc = 2 * col
    n_ch = n_dev // 2
    zc = d_model // 4
    me = lax.axis_index("data")
    chip, core = me // 2, me % 2

    barrier = pltpu.get_barrier_semaphore()
    for k in range(1, n_dev):
        pl.semaphore_signal(barrier, inc=1, device_id=(xor(me, k),), device_id_type=MESH)

    def w1_load(i):
        cols = pl.ds(pl.multiple_of(i * fc, fc), fc)
        return pltpu.make_async_copy(w1_hbm.at[:, cols], w1b.at[pl.ds(0, d_model), cols], load_sem.at[i])

    def w2_load(i):
        cols = pl.ds(pl.multiple_of(i * zc, zc), zc)
        return pltpu.make_async_copy(w2_hbm.at[:, cols], w2.at[:, cols], load_sem.at[n_ch + i])

    base = n_ch + 4
    load_x = pltpu.make_async_copy(x_hbm, xu.at[:, pl.ds(0, d_model)], load_sem.at[base])
    load_a = pltpu.make_async_copy(a_hbm, a_v, load_sem.at[base + 1])
    load_b = pltpu.make_async_copy(b_hbm, w1b.at[pl.ds(d_model, rank), :], load_sem.at[base + 2])
    load_h = pltpu.make_async_copy(head_hbm, head_v, load_sem.at[base + 3])
    load_l = pltpu.make_async_copy(lab_hbm, lab_v, load_sem.at[base + 4])
    load_x.start()
    load_a.start()
    w1_load(0).start()
    load_b.start()
    w1_load(1).start()
    load_h.start()
    load_l.start()
    w1_load(2).start()
    w1_load(3).start()

    pad = xu.shape[1] - d_model
    xu[:, d_model:] = jnp.zeros((tok, pad), BF)
    w1b[d_model + rank:, :] = jnp.zeros((pad - rank, d_ff), BF)
    du_t[...] = jnp.zeros_like(du_t)
    load_x.wait()
    load_a.wait()
    low = mm(xu[:, :d_model], a_v[...], NT)
    xu[:, d_model:d_model + rank] = low.astype(BF)
    u_t[...] = low.T.astype(BF)

    def pre(i):
        w1_load(i).wait()

        @pl.when(i < n_ch // 2)
        def _():
            w1_load(i + n_ch // 2).start()

        @pl.when(i >= n_ch // 2)
        def _():
            w2_load(i - n_ch // 2).start()

        cols = pl.ds(pl.multiple_of(i * fc, fc), fc)
        p = mm(xu[...], w1b[:, cols])
        for r in range(0, tok, 16):
            rs = pl.ds(r, 16)
            x = p[r:r + 16]
            x2 = x * x
            t = jnp.tanh(x * (GELU_C + (GELU_C * GELU_A) * x2))
            hx = 0.5 * x
            t1 = 1.0 + t
            act[rs, cols] = (hx * t1).astype(BF)
            slope[i, rs, :] = 0.5 * t1 + (hx * (1.0 - t * t)) * (GELU_C + (3.0 * GELU_C * GELU_A) * x2)

    load_b.wait()

    def fwd(j, _):
        pre(2 * j)
        pre(2 * j + 1)
        return 0

    lax.fori_loop(0, n_ch // 2, fwd, 0)

    load_h.wait()
    load_l.wait()
    head_t[...] = jnp.zeros_like(head_t)
    for t in range(2):
        head_t[32 * t:32 * t + n_cls, :] = head_v[:, t, :]

    def out_block(i, _):
        w2_load(i).wait()
        cols = pl.ds(pl.multiple_of(i * zc, zc), zc)
        z[:, cols] = (xu[:, cols].astype(F32) + mm(act[...], w2[:, cols])).astype(BF)
        return 0

    lax.fori_loop(0, 4, out_block, 0)

    logits = mm(head_t[...], z[...], NT)
    rows = lax.broadcasted_iota(jnp.int32, (32, tok), 0)
    for t in range(2):
        lg = jnp.where(rows < n_cls, logits[32 * t:32 * t + 32], -jnp.inf)
        ex = jnp.exp(lg - jnp.max(lg, axis=0, keepdims=True))
        prob = ex / jnp.sum(ex, axis=0, keepdims=True)
        err = (prob - (rows == lab_v[t:t + 1, :]).astype(F32)).astype(BF)
        dz[tok * t:tok * t + tok, :] = mm(err, head_t[32 * t:32 * t + 32, :], TN).astype(BF)

    pl.semaphore_wait(barrier, n_dev - 1)

    def chunk_of(kk):
        return xor(chip, kk)

    def d_pre(kk, dp_ref):
        c = chunk_of(kk)
        dh = mm(dz[...], w2[pl.ds(pl.multiple_of(c * fc, fc), fc), :], NT)
        sl = slope[c]
        for t in range(2):
            dp_ref[tok * t:tok * t + tok, :] = (dh[tok * t:tok * t + tok] * sl).astype(BF)

    def b_copy(kk, half):
        dst_core = half
        k = 2 * kk + (core + half) % 2
        return pltpu.make_async_remote_copy(
            src_ref=send_b.at[kk, half], dst_ref=recv_b.at[k], send_sem=sb_sem.at[k], recv_sem=rb_sem.at[k],
            device_id=(2 * chunk_of(kk) + dst_core,), device_id_type=MESH)

    def grads(kk, dp_ref):
        c = chunk_of(kk)
        for t in range(2):
            gb = mm(u_t[...], dp_ref[tok * t:tok * t + tok, :])
            for half in range(2):
                send_b[kk, half, t] = gb[:, col * half:col * half + col]
        bm = w1b[pl.ds(d_model, rank), pl.ds(pl.multiple_of(c * fc, fc), fc)]
        du_t[...] += mm(bm, dp_ref[...], NT)

    d_pre(n_ch - 1, dp0)

    def bwd(j, _):
        kk = n_ch - 1 - 2 * j
        d_pre(kk - 1, dp1)
        grads(kk, dp0)
        b_copy(kk, 0).start()
        b_copy(kk, 1).start()
        d_pre(kk - 2, dp0)
        grads(kk - 1, dp1)
        b_copy(kk - 1, 0).start()
        b_copy(kk - 1, 1).start()
        return 0

    lax.fori_loop(0, n_ch // 2 - 1, bwd, 0)
    d_pre(0, dp1)
    grads(1, dp0)
    b_copy(1, 0).start()
    b_copy(1, 1).start()
    grads(0, dp1)
    b_copy(0, 1 - core).start()

    lane = lax.broadcasted_iota(jnp.int32, (rank, 128), 1)
    ga = [mm(du_t[:, tok * t:tok * t + tok].astype(BF), xu[:, :d_model]) for t in range(2)]
    for j in range(n_ch):
        a0, a1 = (ga[t][:, 128 * j:128 * j + 128] for t in range(2))
        send_a[2 * j] = jnp.where(lane < 64, a0, pltpu.roll(a1, 64, 1))
        send_a[2 * j + 1] = jnp.where(lane < 64, pltpu.roll(a0, 64, 1), a1)

    def a_copy(k):
        dst = xor(me, k)
        return pltpu.make_async_remote_copy(
            src_ref=send_a.at[dst], dst_ref=recv_a.at[k], send_sem=sa_sem.at[k], recv_sem=ra_sem.at[k],
            device_id=(dst,), device_id_type=MESH)

    def m_copy(k):
        return pltpu.make_async_remote_copy(
            src_ref=send_m, dst_ref=recv_m.at[k], send_sem=sm_sem.at[k], recv_sem=rm_sem.at[k],
            device_id=(xor(me, k),), device_id_type=MESH)

    order = [15, 14, 13, 11, 10, 7, 6, 12, 9, 5, 3, 8, 4, 2, 1]
    for k in order:
        a_copy(k).start()

    def b_half(k):
        return b_copy(k // 2, (core + k) % 2)

    sum_b = send_b[0, core]
    for k in reversed(range(1, n_dev)):
        b_half(k).wait_recv()
        sum_b = sum_b + recv_b[k]
    sum_b = sum_b * (1.0 / total)
    b0, b1 = sum_b[0], sum_b[1]
    sq0, sq1, cross = b0 * b0, b1 * b1, b0 * b1
    sum_a = send_a[me]
    for k in reversed(order):
        a_copy(k).wait_recv()
        sum_a = sum_a + recv_a[k]
    sum_a = sum_a * (1.0 / total)
    sq = sum_a * sum_a
    sign = jnp.where(lane < 64, 1.0, -1.0)
    other = pltpu.roll(sum_a, 64, 1)

    def fold(part_b, part_a):
        return jnp.sum(part_b[:, :128] + part_b[:, 128:] + part_a, axis=0, keepdims=True)

    diff = fold(sq0 - sq1, sq * sign)
    both = fold(sq0 + sq1, sq)
    mix = fold(cross, 0.5 * sum_a * other)
    send_m[0:1, :] = diff
    send_m[1:2, :] = both
    send_m[2:3, :] = mix
    send_m[3:4, :] = jnp.zeros_like(mix)
    for k in order:
        m_copy(k).start()
    sum_m = send_m[...]
    for k in reversed(order):
        m_copy(k).wait_recv()
        sum_m = sum_m + recv_m[k]
    gram = jnp.broadcast_to(jnp.sum(sum_m, axis=1, keepdims=True), sum_m.shape)
    m_diff, m_both, m_mix = gram[0:1], gram[1:2], gram[2:3]
    scale = 0.5 / m_both
    c0 = m_diff * scale
    c1 = (m_both - 2.0 * m_mix) * scale
    e = jnp.zeros_like(c0)
    for _ in range(EG_STEPS):
        e = e - (c0 + c1 * jnp.tanh(e))
    al0 = 1.0 / (1.0 + jnp.exp(-2.0 * e))
    al1 = 1.0 / (1.0 + jnp.exp(2.0 * e))
    gb_ref[...] = al0[:, 0:1] * b0 + al1[:, 0:1] * b1
    ga_ref[...] = (al0 * sum_a + al1 * other)[:, :64]
    alpha_ref[...] = jnp.where(lane[0:1, :] == 0, al0, al1)[:, 0:2]
    for k in range(1, n_dev):
        b_half(k).wait_send()
        a_copy(k).wait_send()
        m_copy(k).wait_send()


def finish(alpha_in, ga_in, gb_in, alpha_ref, ga_ref, gb_ref):
    alpha_ref[...] = alpha_in[...]
    ga_ref[...] = ga_in[...]
    gb_ref[...] = gb_in[...]


def solution(mesh):
    n_dev = mesh.shape["data"]

    def device_step(tokens, labels, w_one, w_two, adapter_a, adapter_b, task_heads):
        tok, d_model = tokens.shape
        d_ff = w_one.shape[1]
        rank = adapter_a.shape[1]
        n_tasks, _, n_cls = task_heads.shape
        col = d_ff // n_dev
        fc = 2 * col
        dma = pltpu.SemaphoreType.DMA
        alpha, ga, gb = pl.pallas_call(
            functools.partial(kernel, (n_dev, tok * n_dev)),
            out_shape=(
                jax.ShapeDtypeStruct((1, n_tasks), F32),
                jax.ShapeDtypeStruct((rank, d_model // n_dev), F32),
                jax.ShapeDtypeStruct((rank, col), F32),
            ),
            in_specs=[pl.BlockSpec(memory_space=pl.ANY)] * 7,
            out_specs=[pl.BlockSpec(memory_space=pltpu.VMEM)] * 3,
            scratch_shapes=[
                pltpu.VMEM((tok, d_model + 128), BF),
                pltpu.VMEM((d_model + 128, d_ff), BF),
                pltpu.VMEM((d_ff, d_model), BF),
                pltpu.VMEM((rank, d_model), BF),
                pltpu.VMEM((n_cls, n_tasks, d_model), BF),
                pltpu.VMEM((n_tasks, tok), jnp.int32),
                pltpu.VMEM((n_tasks * 32, d_model), BF),
                pltpu.VMEM((rank, tok), BF),
                pltpu.VMEM((tok, fc), F32),
                pltpu.VMEM((tok, fc), F32),
                pltpu.VMEM((tok, d_ff), BF),
                pltpu.VMEM((n_dev // 2, tok, fc), F32),
                pltpu.VMEM((tok, d_model), BF),
                pltpu.VMEM((n_tasks * tok, d_model), BF),
                pltpu.VMEM((n_tasks * tok, fc), BF),
                pltpu.VMEM((n_tasks * tok, fc), BF),
                pltpu.VMEM((rank, n_tasks * tok), F32),
                pltpu.VMEM((n_dev // 2, 2, n_tasks, rank, col), F32),
                pltpu.VMEM((n_dev, n_tasks, rank, col), F32),
                pltpu.VMEM((n_dev, rank, 128), F32),
                pltpu.VMEM((n_dev, rank, 128), F32),
                pltpu.VMEM((4, 128), F32),
                pltpu.VMEM((n_dev, 4, 128), F32),
                dma((n_dev // 2 + 9,)),
                dma((n_dev,)), dma((n_dev,)), dma((n_dev,)), dma((n_dev,)), dma((n_dev,)), dma((n_dev,)),
            ],
            compiler_params=pltpu.CompilerParams(collective_id=0, has_side_effects=True, vmem_limit_bytes=60 * 1024 * 1024),
            name="step",
        )(tokens, labels, w_one, w_two, adapter_a.T, adapter_b, task_heads.transpose(2, 0, 1))
        outs = (alpha, ga, gb)
        alpha, ga, gb = pl.pallas_call(
            finish,
            out_shape=[jax.ShapeDtypeStruct(o.shape, o.dtype) for o in outs],
            in_specs=[pl.BlockSpec(memory_space=pltpu.VMEM)] * 3,
            out_specs=[pl.BlockSpec(memory_space=pltpu.VMEM)] * 3,
            name="finish",
        )(*outs)
        return alpha.reshape(n_tasks), ga.T, gb

    return jax.shard_map(device_step, mesh=mesh, in_specs=(P("data", None), P(None, "data"), P(), P(), P(), P(), P()), out_specs=(P(), P("data", None), P(None, "data")), check_vma=False)
```

```python
import functools

import jax
import jax.numpy as jnp
from jax import lax
from jax.experimental import pallas as pl
from jax.experimental.pallas import tpu as pltpu
from jax.sharding import PartitionSpec as P

EG_STEPS = 20
BF = jnp.bfloat16
F32 = jnp.float32
GELU_C = 0.7978845608028654
GELU_A = 0.044715
MESH = pl.DeviceIdType.MESH
BITS = (1, 2, 4, 8)
STRIP = 32
NT = (((1,), (1,)), ((), ()))
TN = (((0,), (0,)), ((), ()))


def xor(a, b):
    return sum(bit * ((a // bit + b // bit) % 2) for bit in BITS)


def mm(a, b, dims=(((1,), (0,)), ((), ()))):
    return lax.dot_general(a, b, dims, preferred_element_type=F32)


def kernel(cfg, x_hbm, lab_hbm, w1_hbm, w2_hbm, a_hbm, b_hbm, head_hbm, alpha_ref, ga_ref, gb_ref, xu, w1b, w2, a_v, head_v, lab_v, head_t, u_t, act, slope, z, dz, dp0, dp1, du_t, send_b, recv_b, send_a, recv_a, send_m, recv_m, load_sem, sb_sem, rb_sem, sa_sem, ra_sem, sm_sem, rm_sem):
    n_dev, total = cfg
    tok, d_model = x_hbm.shape
    d_ff = w1_hbm.shape[1]
    rank = a_hbm.shape[0]
    n_cls, n_task = head_hbm.shape[0], head_hbm.shape[1]
    col = d_ff // n_dev
    fc = 2 * col
    n_ch = n_dev // 2
    me = lax.axis_index("data")
    chip, core = me // 2, me % 2

    barrier = pltpu.get_barrier_semaphore()
    for k in range(1, n_dev):
        pl.semaphore_signal(barrier, inc=1, device_id=(xor(me, k),), device_id_type=MESH)

    sem_at = [0]

    def load(src, dst):
        copy = pltpu.make_async_copy(src, dst, load_sem.at[sem_at[0]])
        sem_at[0] += 1
        copy.start()
        return copy

    load_h = load(head_hbm, head_v)
    load_a = load(a_hbm, a_v)
    load_x = load(x_hbm, xu.at[:, pl.ds(0, d_model)])
    load_b = load(b_hbm, w1b.at[pl.ds(d_model, rank), :])
    load_w1 = [load(w1_hbm.at[:, pl.ds(i * fc, fc)], w1b.at[pl.ds(0, d_model), pl.ds(i * fc, fc)]) for i in range(n_ch)]
    load_l = load(lab_hbm, lab_v)
    w2_rows = d_ff // 4
    load_w2 = [load(w2_hbm.at[pl.ds(i * w2_rows, w2_rows), :], w2.at[pl.ds(i * w2_rows, w2_rows), :]) for i in range(4)]

    pad = xu.shape[1] - d_model
    xu[:, d_model:] = jnp.zeros((tok, pad), BF)
    w1b[d_model + rank:, :] = jnp.zeros((pad - rank, d_ff), BF)
    head_t[...] = jnp.zeros_like(head_t)
    du_t[...] = jnp.zeros_like(du_t)
    load_h.wait()
    for t in range(n_task):
        head_t[32 * t:32 * t + n_cls, :] = head_v[:, t, :]
    load_a.wait()
    load_b.wait()
    load_x.wait()
    load_w1[0].wait()
    low = mm(xu[:, :d_model], a_v[...], NT)
    xu[:, d_model:d_model + rank] = low.astype(BF)
    u_t[...] = low.T.astype(BF)

    def pre(i):
        slope[i] = mm(xu[...], w1b[:, i * fc:i * fc + fc])

    def gelu(i):
        cols = slice(i * fc, i * fc + fc)
        for r in range(0, tok, STRIP):
            rs = slice(r, r + STRIP)
            x = slope[i, rs, :]
            x2 = x * x
            t = jnp.tanh(x * (GELU_C + (GELU_C * GELU_A) * x2))
            t1 = 1.0 + t
            g = (0.5 * x) * t1
            act[rs, cols] = g.astype(BF)
            slope[i, rs, :] = 0.5 * t1 + (g * (1.0 - t)) * (GELU_C + (3.0 * GELU_C * GELU_A) * x2)

    waits = {1: (1, 2), 3: tuple(range(3, n_ch))}
    for i in range(n_ch):
        for w in waits.get(i, ()):
            load_w1[w].wait()
        pre(i)
        if i:
            gelu(i - 1)
    for w in load_w2:
        w.wait()
    load_l.wait()
    gelu(n_ch - 1)
    zc = d_model // 2
    for n in range(2):
        cs = slice(n * zc, n * zc + zc)
        zz = mm(act[...], w2[:, cs])
        for r in range(0, tok, STRIP):
            rs = slice(r, r + STRIP)
            z[rs, cs] = (xu[rs, cs].astype(F32) + zz[rs]).astype(BF)

    logits = mm(head_t[...], z[...], NT)
    rows = lax.broadcasted_iota(jnp.int32, (32, tok), 0)
    for t in range(n_task):
        lg = jnp.where(rows < n_cls, logits[32 * t:32 * t + 32], -jnp.inf)
        ex = jnp.exp(lg - jnp.max(lg, axis=0, keepdims=True))
        prob = ex / jnp.sum(ex, axis=0, keepdims=True)
        err = (prob - (rows == lab_v[t:t + 1, :]).astype(F32)).astype(BF)
        dz[tok * t:tok * t + tok, :] = mm(err, head_t[32 * t:32 * t + 32, :], TN).astype(BF)

    pl.semaphore_wait(barrier, n_dev - 1)

    def chunk_of(kk):
        return xor(chip, kk)

    def b_copy(t, kk, half):
        k = 2 * kk + (core + half) % 2
        return pltpu.make_async_remote_copy(
            src_ref=send_b.at[t, kk, half], dst_ref=recv_b.at[t, k - 1], send_sem=sb_sem.at[t], recv_sem=rb_sem.at[t],
            device_id=(2 * chunk_of(kk) + half,), device_id_type=MESH)

    def a_copy(t, k):
        dst = xor(me, k)
        return pltpu.make_async_remote_copy(
            src_ref=send_a.at[t, dst], dst_ref=recv_a.at[t, k - 1], send_sem=sa_sem.at[t], recv_sem=ra_sem.at[t],
            device_id=(dst,), device_id_type=MESH)

    def m_copy(k):
        return pltpu.make_async_remote_copy(
            src_ref=send_m, dst_ref=recv_m.at[k - 1], send_sem=sm_sem.at[0], recv_sem=rm_sem.at[0],
            device_id=(xor(me, k),), device_id_type=MESH)

    order = [15, 14, 13, 11, 10, 7, 6, 12, 9, 5, 3, 8, 4, 2, 1]
    lane8 = lax.broadcasted_iota(jnp.int32, (8, 128), 1)

    def wait_all(ref, sem):
        pltpu.make_async_copy(ref, ref, sem).wait()

    def d_pre(j, dp_ref):
        t, c = j // n_ch, chunk_of(n_ch - 1 - j % n_ch)
        dh = mm(dz[pl.ds(pl.multiple_of(t * tok, tok), tok), :], w2[pl.ds(pl.multiple_of(c * fc, fc), fc), :], NT)
        for r in range(0, tok, STRIP):
            rs = slice(r, r + STRIP)
            dp_ref[rs, :] = (dh[rs] * slope[c, rs, :]).astype(BF)

    def grads(j, dp_ref):
        t, kk = j // n_ch, n_ch - 1 - j % n_ch
        c = chunk_of(kk)
        bm = w1b[pl.ds(d_model, rank), pl.ds(pl.multiple_of(c * fc, fc), fc)]
        du_t[t] += mm(bm, dp_ref[...], NT)
        gb = mm(u_t[...], dp_ref[...])
        for half in range(2):
            send_b[t, kk, half] = gb[:, col * half:col * half + col]
        return t, kk

    def low_grad(t):
        ga = mm(du_t[t].astype(BF), xu[:, :d_model])
        for j in range(n_ch):
            top, low = ga[0:8, 128 * j:128 * j + 128], ga[8:16, 128 * j:128 * j + 128]
            send_a[t, 2 * j] = jnp.where(lane8 < 64, top, pltpu.roll(low, 64, 1))
            send_a[t, 2 * j + 1] = jnp.where(lane8 < 64, pltpu.roll(top, 64, 1), low)
        for k in order:
            a_copy(t, k).start()

    n_unit = n_task * n_ch
    d_pre(0, dp0)

    def bwd(i, _):
        d_pre(2 * i + 1, dp1)
        t, kk = grads(2 * i, dp0)
        d_pre(2 * i + 2, dp0)
        b_copy(t, kk, 0).start()
        b_copy(t, kk, 1).start()
        t, kk = grads(2 * i + 1, dp1)

        @pl.when(i != n_ch // 2 - 1)
        def _():
            b_copy(t, kk, 0).start()
            b_copy(t, kk, 1).start()

        @pl.when(i == n_ch // 2 - 1)
        def _():
            b_copy(0, 0, 1 - core).start()
            low_grad(0)

        return 0

    lax.fori_loop(0, n_unit // 2 - 1, bwd, 0)
    d_pre(n_unit - 1, dp1)
    t, kk = grads(n_unit - 2, dp0)
    b_copy(t, kk, 0).start()
    b_copy(t, kk, 1).start()
    grads(n_unit - 1, dp1)
    low_grad(1)
    b_copy(1, 0, 1 - core).start()

    inv = 1.0 / total

    def sum_up(own, recv, sem):
        wait_all(recv, sem)
        s = own
        for k in range(n_dev - 1):
            s = s + recv[k]
        return s * inv

    b_sum = [sum_up(send_b[t, 0, core], recv_b.at[t], rb_sem.at[t]) for t in range(n_task)]
    a_sum = [sum_up(send_a[t, me], recv_a.at[t], ra_sem.at[t]) for t in range(n_task)]

    def fold(part_b, part_a):
        return jnp.sum(part_b[:8, :128] + part_b[:8, 128:] + part_b[8:, :128] + part_b[8:, 128:] + part_a, axis=0, keepdims=True)

    b0, b1 = b_sum
    a0, a1 = a_sum
    s0 = fold(b0 * b0, a0 * a0)
    s1 = fold(b1 * b1, a1 * a1)
    mix = fold(b0 * b1, a0 * a1)
    send_m[0:1, :] = s0 - s1
    send_m[1:2, :] = s0 + s1
    send_m[2:3, :] = mix
    send_m[3:4, :] = jnp.zeros_like(mix)
    for k in order:
        m_copy(k).start()
    sum_m = send_m[...]
    wait_all(recv_m, rm_sem.at[0])
    for k in range(n_dev - 1):
        sum_m = sum_m + recv_m[k]
    gram = jnp.broadcast_to(jnp.sum(sum_m, axis=1, keepdims=True), sum_m.shape)
    m_diff, m_both, m_mix = gram[0:1], gram[1:2], gram[2:3]
    scale = 0.5 / m_both
    c0 = m_diff * scale
    c1 = (m_both - 2.0 * m_mix) * scale
    e = jnp.zeros_like(c0)
    for _ in range(EG_STEPS):
        e = e - (c0 + c1 * jnp.tanh(e))
    al0 = 1.0 / (1.0 + jnp.exp(-2.0 * e))
    al1 = 1.0 / (1.0 + jnp.exp(2.0 * e))
    gb_ref[...] = al0[:, 0:1] * b0 + al1[:, 0:1] * b1
    comb = al0 * a0 + al1 * a1
    ga_ref[0:8, :] = comb[:, :64]
    ga_ref[8:16, :] = pltpu.roll(comb, 64, 1)[:, :64]
    alpha_ref[...] = jnp.where(lane8[0:1, :] == 0, al0, al1)[:, 0:2]
    for t in range(n_task):
        wait_all(recv_b.at[t], sb_sem.at[t])
        wait_all(recv_a.at[t], sa_sem.at[t])
    wait_all(recv_m, sm_sem.at[0])


def finish(alpha_in, ga_in, gb_in, alpha_ref, ga_ref, gb_ref):
    alpha_ref[...] = alpha_in[...]
    ga_ref[...] = ga_in[...]
    gb_ref[...] = gb_in[...]


def solution(mesh):
    n_dev = mesh.shape["data"]

    def device_step(tokens, labels, w_one, w_two, adapter_a, adapter_b, task_heads):
        tok, d_model = tokens.shape
        d_ff = w_one.shape[1]
        rank = adapter_a.shape[1]
        n_tasks, _, n_cls = task_heads.shape
        col = d_ff // n_dev
        fc = 2 * col
        dma = pltpu.SemaphoreType.DMA
        outs = pl.pallas_call(
            functools.partial(kernel, (n_dev, tok * n_dev)),
            out_shape=(
                jax.ShapeDtypeStruct((1, n_tasks), F32),
                jax.ShapeDtypeStruct((rank, d_model // n_dev), F32),
                jax.ShapeDtypeStruct((rank, col), F32),
            ),
            in_specs=[pl.BlockSpec(memory_space=pl.ANY)] * 7,
            out_specs=[pl.BlockSpec(memory_space=pltpu.VMEM)] * 3,
            scratch_shapes=[
                pltpu.VMEM((tok, d_model + 128), BF),
                pltpu.VMEM((d_model + 128, d_ff), BF),
                pltpu.VMEM((d_ff, d_model), BF),
                pltpu.VMEM((rank, d_model), BF),
                pltpu.VMEM((n_cls, n_tasks, d_model), BF),
                pltpu.VMEM((n_tasks, tok), jnp.int32),
                pltpu.VMEM((n_tasks * 32, d_model), BF),
                pltpu.VMEM((rank, tok), BF),
                pltpu.VMEM((tok, d_ff), BF),
                pltpu.VMEM((n_dev // 2, tok, fc), F32),
                pltpu.VMEM((tok, d_model), BF),
                pltpu.VMEM((n_tasks * tok, d_model), BF),
                pltpu.VMEM((tok, fc), BF),
                pltpu.VMEM((tok, fc), BF),
                pltpu.VMEM((n_tasks, rank, tok), F32),
                pltpu.VMEM((n_tasks, n_dev // 2, 2, rank, col), F32),
                pltpu.VMEM((n_tasks, n_dev - 1, rank, col), F32),
                pltpu.VMEM((n_tasks, n_dev, 8, 128), F32),
                pltpu.VMEM((n_tasks, n_dev - 1, 8, 128), F32),
                pltpu.VMEM((4, 128), F32),
                pltpu.VMEM((n_dev - 1, 4, 128), F32),
                dma((n_dev // 2 + 9,)),
                dma((n_tasks,)), dma((n_tasks,)), dma((n_tasks,)), dma((n_tasks,)), dma((1,)), dma((1,)),
            ],
            compiler_params=pltpu.CompilerParams(collective_id=0, has_side_effects=True, vmem_limit_bytes=60 * 1024 * 1024),
            name="step",
        )(tokens, labels, w_one, w_two, adapter_a.T, adapter_b, task_heads.transpose(2, 0, 1))
        alpha, ga, gb = pl.pallas_call(
            finish,
            out_shape=[jax.ShapeDtypeStruct(o.shape, o.dtype) for o in outs],
            in_specs=[pl.BlockSpec(memory_space=pltpu.VMEM)] * 3,
            out_specs=[pl.BlockSpec(memory_space=pltpu.VMEM)] * 3,
            name="finish",
        )(*outs)
        return alpha.reshape(n_tasks), ga.T, gb

    return jax.shard_map(device_step, mesh=mesh, in_specs=(P("data", None), P(None, "data"), P(), P(), P(), P(), P()), out_specs=(P(), P("data", None), P(None, "data")), check_vma=False)
```

```python
import functools

import jax
import jax.numpy as jnp
from jax import lax
from jax.experimental import pallas as pl
from jax.experimental.pallas import tpu as pltpu
from jax.sharding import PartitionSpec as P

EG_STEPS = 20
BF = jnp.bfloat16
F32 = jnp.float32
GELU_C = 0.7978845608028654
GELU_A = 0.044715
MESH = pl.DeviceIdType.MESH
BITS = (1, 2, 4, 8)
STRIP = 32
NT = (((1,), (1,)), ((), ()))
TN = (((0,), (0,)), ((), ()))


def xor(a, b):
    return sum(bit * ((a // bit + b // bit) % 2) for bit in BITS)


def mm(a, b, dims=(((1,), (0,)), ((), ()))):
    return lax.dot_general(a, b, dims, preferred_element_type=F32)


def kernel(cfg, x_hbm, lab_hbm, w1_hbm, w2_hbm, a_hbm, b_hbm, head_hbm, alpha_ref, ga_ref, gb_ref, xu, w1b, w2, a_v, head_v, lab_v, head_t, u_t, act, slope, z, dz, dp0, dp1, du_t, send_b, recv_b, send_a, recv_a, send_m, recv_m, load_sem, sb_sem, rb_sem, sa_sem, ra_sem, sm_sem, rm_sem):
    n_dev, total = cfg
    tok, d_model = x_hbm.shape
    d_ff = w1_hbm.shape[1]
    rank = a_hbm.shape[0]
    n_cls, n_task = head_hbm.shape[0], head_hbm.shape[1]
    col = d_ff // n_dev
    fc = 2 * col
    n_ch = n_dev // 2
    me = lax.axis_index("data")
    chip, core = me // 2, me % 2

    barrier = pltpu.get_barrier_semaphore()
    for k in range(1, n_dev):
        pl.semaphore_signal(barrier, inc=1, device_id=(xor(me, k),), device_id_type=MESH)

    sem_at = [0]

    def load(src, dst):
        copy = pltpu.make_async_copy(src, dst, load_sem.at[sem_at[0]])
        sem_at[0] += 1
        copy.start()
        return copy

    load_h = load(head_hbm, head_v)
    load_a = load(a_hbm, a_v)
    load_x = load(x_hbm, xu.at[:, pl.ds(0, d_model)])
    load_b = load(b_hbm, w1b.at[pl.ds(d_model, rank), :])
    load_w1 = [load(w1_hbm.at[:, pl.ds(i * fc, fc)], w1b.at[pl.ds(0, d_model), pl.ds(i * fc, fc)]) for i in range(n_ch)]
    load_l = load(lab_hbm, lab_v)
    w2_rows = d_ff // 4
    load_w2 = [load(w2_hbm.at[pl.ds(i * w2_rows, w2_rows), :], w2.at[pl.ds(i * w2_rows, w2_rows), :]) for i in range(4)]

    pad = xu.shape[1] - d_model
    xu[:, d_model:] = jnp.zeros((tok, pad), BF)
    w1b[d_model + rank:, :] = jnp.zeros((pad - rank, d_ff), BF)
    head_t[...] = jnp.zeros_like(head_t)
    load_h.wait()
    for t in range(n_task):
        head_t[32 * t:32 * t + n_cls, :] = head_v[:, t, :]
    load_a.wait()
    load_b.wait()
    load_x.wait()
    load_w1[0].wait()
    low = mm(xu[:, :d_model], a_v[...], NT)
    xu[:, d_model:d_model + rank] = low.astype(BF)
    u_t[...] = low.T.astype(BF)

    def pre(i):
        slope[i] = mm(xu[...], w1b[:, i * fc:i * fc + fc])

    def gelu(i):
        cols = slice(i * fc, i * fc + fc)
        for r in range(0, tok, STRIP):
            rs = slice(r, r + STRIP)
            x = slope[i, rs, :]
            x2 = x * x
            t = jnp.tanh(x * (GELU_C + (GELU_C * GELU_A) * x2))
            t1 = 1.0 + t
            g = (0.5 * x) * t1
            act[rs, cols] = g.astype(BF)
            slope[i, rs, :] = 0.5 * t1 + (g * (1.0 - t)) * (GELU_C + (3.0 * GELU_C * GELU_A) * x2)

    def stage(first, last):
        @pl.when(me >= 0)
        def _():
            for i in range(first, last):
                pre(i)
                if i:
                    gelu(i - 1)

    stage(0, 1)
    for w in load_w1[1:3]:
        w.wait()
    stage(1, 3)
    for w in load_w1[3:]:
        w.wait()
    stage(3, n_ch)
    for w in load_w2:
        w.wait()
    load_l.wait()
    hl = tok // 2
    zc = d_model // 2

    def out_block(h, n):
        cs = slice(n * zc, n * zc + zc)
        zz = mm(act[h * hl:h * hl + hl, :], w2[:, cs])
        for r in range(0, hl, STRIP):
            rs = slice(h * hl + r, h * hl + r + STRIP)
            z[rs, cs] = (xu[rs, cs].astype(F32) + zz[r:r + STRIP]).astype(BF)

    def errors(h):
        hs = slice(h * hl, h * hl + hl)
        logits = mm(head_t[...], z[hs, :], NT)
        rows = lax.broadcasted_iota(jnp.int32, (32, hl), 0)
        out = []
        for t in range(n_task):
            lg = jnp.where(rows < n_cls, logits[32 * t:32 * t + 32], -jnp.inf)
            ex = jnp.exp(lg - jnp.max(lg, axis=0, keepdims=True))
            prob = ex / jnp.sum(ex, axis=0, keepdims=True)
            out.append((prob - (rows == lab_v[t:t + 1, hs]).astype(F32)).astype(BF))
        return out

    def d_trunk(h, errs):
        for t in range(n_task):
            dz[tok * t + h * hl:tok * t + h * hl + hl, :] = mm(errs[t], head_t[32 * t:32 * t + 32, :], TN).astype(BF)

    @pl.when(me >= 0)
    def _():
        gelu(n_ch - 1)
        out_block(0, 0)
        out_block(0, 1)
        out_block(1, 0)
        errs0 = errors(0)
        out_block(1, 1)
        errs1 = errors(1)
        d_trunk(0, errs0)
        d_trunk(1, errs1)

    pl.semaphore_wait(barrier, n_dev - 1)

    def chunk_of(kk):
        return xor(chip, kk)

    def b_copy(t, kk, half):
        k = 2 * kk + (core + half) % 2
        return pltpu.make_async_remote_copy(
            src_ref=send_b.at[t, kk, half], dst_ref=recv_b.at[t, k - 1], send_sem=sb_sem.at[t], recv_sem=rb_sem.at[t],
            device_id=(2 * chunk_of(kk) + half,), device_id_type=MESH)

    def a_copy(t, k):
        dst = xor(me, k)
        return pltpu.make_async_remote_copy(
            src_ref=send_a.at[t, dst], dst_ref=recv_a.at[t, k - 1], send_sem=sa_sem.at[t], recv_sem=ra_sem.at[t],
            device_id=(dst,), device_id_type=MESH)

    def m_copy(k):
        return pltpu.make_async_remote_copy(
            src_ref=send_m, dst_ref=recv_m.at[k - 1], send_sem=sm_sem.at[0], recv_sem=rm_sem.at[0],
            device_id=(xor(me, k),), device_id_type=MESH)

    order = [15, 14, 13, 11, 10, 7, 6, 12, 9, 5, 3, 8, 4, 2, 1]
    lane8 = lax.broadcasted_iota(jnp.int32, (8, 128), 1)

    def wait_all(ref, sem):
        pltpu.make_async_copy(ref, ref, sem).wait()

    def d_pre(t, kk, dp_ref):
        c = chunk_of(kk)
        dh = mm(dz[pl.ds(pl.multiple_of(t * tok, tok), tok), :], w2[pl.ds(pl.multiple_of(c * fc, fc), fc), :], NT)
        for r in range(0, tok, STRIP):
            rs = slice(r, r + STRIP)
            dp_ref[rs, :] = (dh[rs] * slope[c, rs, :]).astype(BF)

    def grads(t, kk, dp_ref):
        c = chunk_of(kk)
        bm = w1b[pl.ds(d_model, rank), pl.ds(pl.multiple_of(c * fc, fc), fc)]
        part = mm(bm, dp_ref[...], NT)
        du_t[...] = part if kk == n_ch - 1 else du_t[...] + part
        gb = mm(u_t[...], dp_ref[...])
        for half in range(2):
            send_b[t, kk, half] = gb[:, col * half:col * half + col]

    def low_grad(t):
        ga = mm(du_t[...].astype(BF), xu[:, :d_model])
        for j in range(n_ch):
            top, low = ga[0:8, 128 * j:128 * j + 128], ga[8:16, 128 * j:128 * j + 128]
            send_a[t, 2 * j] = jnp.where(lane8 < 64, top, pltpu.roll(low, 64, 1))
            send_a[t, 2 * j + 1] = jnp.where(lane8 < 64, pltpu.roll(top, 64, 1), low)
        for k in order:
            a_copy(t, k).start()

    def task(t, _):
        dps = (dp0, dp1)
        d_pre(t, n_ch - 1, dps[1])
        for kk in reversed(range(n_ch)):
            if kk:
                d_pre(t, kk - 1, dps[(kk - 1) % 2])
            grads(t, kk, dps[kk % 2])
            if kk and kk % 2 == 0:
                for k2 in (kk + 1, kk):
                    b_copy(t, k2, 0).start()
                    b_copy(t, k2, 1).start()
        low_grad(t)
        b_copy(t, 1, 0).start()
        b_copy(t, 1, 1).start()
        b_copy(t, 0, 1 - core).start()
        return 0

    lax.fori_loop(0, n_task, task, 0)

    inv = 1.0 / total

    def sum_up(own, recv, sem):
        wait_all(recv, sem)
        s = own
        for k in range(n_dev - 1):
            s = s + recv[k]
        return s * inv

    b_sum = [sum_up(send_b[t, 0, core], recv_b.at[t], rb_sem.at[t]) for t in range(n_task)]
    a_sum = [sum_up(send_a[t, me], recv_a.at[t], ra_sem.at[t]) for t in range(n_task)]

    def fold(part_b, part_a):
        return jnp.sum(part_b[:8, :128] + part_b[:8, 128:] + part_b[8:, :128] + part_b[8:, 128:] + part_a, axis=0, keepdims=True)

    b0, b1 = b_sum
    a0, a1 = a_sum
    s0 = fold(b0 * b0, a0 * a0)
    s1 = fold(b1 * b1, a1 * a1)
    mix = fold(b0 * b1, a0 * a1)
    send_m[0:1, :] = s0 - s1
    send_m[1:2, :] = s0 + s1
    send_m[2:3, :] = mix
    send_m[3:4, :] = jnp.zeros_like(mix)
    for k in order:
        m_copy(k).start()
    sum_m = send_m[...]
    wait_all(recv_m, rm_sem.at[0])
    for k in range(n_dev - 1):
        sum_m = sum_m + recv_m[k]
    gram = jnp.broadcast_to(jnp.sum(sum_m, axis=1, keepdims=True), sum_m.shape)
    m_diff, m_both, m_mix = gram[0:1], gram[1:2], gram[2:3]
    scale = 0.5 / m_both
    c0 = m_diff * scale
    c1 = (m_both - 2.0 * m_mix) * scale
    e = jnp.zeros_like(c0)
    for _ in range(EG_STEPS):
        e = e - (c0 + c1 * jnp.tanh(e))
    al0 = 1.0 / (1.0 + jnp.exp(-2.0 * e))
    al1 = 1.0 / (1.0 + jnp.exp(2.0 * e))
    gb_ref[...] = al0[:, 0:1] * b0 + al1[:, 0:1] * b1
    comb = al0 * a0 + al1 * a1
    ga_ref[0:8, :] = comb[:, :64]
    ga_ref[8:16, :] = pltpu.roll(comb, 64, 1)[:, :64]
    alpha_ref[...] = jnp.where(lane8[0:1, :] == 0, al0, al1)[:, 0:2]
    for t in range(n_task):
        wait_all(recv_b.at[t], sb_sem.at[t])
        wait_all(recv_a.at[t], sa_sem.at[t])
    wait_all(recv_m, sm_sem.at[0])


def finish(alpha_in, ga_in, gb_in, alpha_ref, ga_ref, gb_ref):
    alpha_ref[...] = alpha_in[...]
    ga_ref[...] = ga_in[...]
    gb_ref[...] = gb_in[...]


def solution(mesh):
    n_dev = mesh.shape["data"]

    def device_step(tokens, labels, w_one, w_two, adapter_a, adapter_b, task_heads):
        tok, d_model = tokens.shape
        d_ff = w_one.shape[1]
        rank = adapter_a.shape[1]
        n_tasks, _, n_cls = task_heads.shape
        col = d_ff // n_dev
        fc = 2 * col
        dma = pltpu.SemaphoreType.DMA
        outs = pl.pallas_call(
            functools.partial(kernel, (n_dev, tok * n_dev)),
            out_shape=(
                jax.ShapeDtypeStruct((1, n_tasks), F32),
                jax.ShapeDtypeStruct((rank, d_model // n_dev), F32),
                jax.ShapeDtypeStruct((rank, col), F32),
            ),
            in_specs=[pl.BlockSpec(memory_space=pl.ANY)] * 7,
            out_specs=[pl.BlockSpec(memory_space=pltpu.VMEM)] * 3,
            scratch_shapes=[
                pltpu.VMEM((tok, d_model + 128), BF),
                pltpu.VMEM((d_model + 128, d_ff), BF),
                pltpu.VMEM((d_ff, d_model), BF),
                pltpu.VMEM((rank, d_model), BF),
                pltpu.VMEM((n_cls, n_tasks, d_model), BF),
                pltpu.VMEM((n_tasks, tok), jnp.int32),
                pltpu.VMEM((n_tasks * 32, d_model), BF),
                pltpu.VMEM((rank, tok), BF),
                pltpu.VMEM((tok, d_ff), BF),
                pltpu.VMEM((n_dev // 2, tok, fc), F32),
                pltpu.VMEM((tok, d_model), BF),
                pltpu.VMEM((n_tasks * tok, d_model), BF),
                pltpu.VMEM((tok, fc), BF),
                pltpu.VMEM((tok, fc), BF),
                pltpu.VMEM((rank, tok), F32),
                pltpu.VMEM((n_tasks, n_dev // 2, 2, rank, col), F32),
                pltpu.VMEM((n_tasks, n_dev - 1, rank, col), F32),
                pltpu.VMEM((n_tasks, n_dev, 8, 128), F32),
                pltpu.VMEM((n_tasks, n_dev - 1, 8, 128), F32),
                pltpu.VMEM((4, 128), F32),
                pltpu.VMEM((n_dev - 1, 4, 128), F32),
                dma((n_dev // 2 + 9,)),
                dma((n_tasks,)), dma((n_tasks,)), dma((n_tasks,)), dma((n_tasks,)), dma((1,)), dma((1,)),
            ],
            compiler_params=pltpu.CompilerParams(collective_id=0, has_side_effects=True, vmem_limit_bytes=60 * 1024 * 1024),
            name="step",
        )(tokens, labels, w_one, w_two, adapter_a.T, adapter_b, task_heads.transpose(2, 0, 1))
        alpha, ga, gb = pl.pallas_call(
            finish,
            out_shape=[jax.ShapeDtypeStruct(o.shape, o.dtype) for o in outs],
            in_specs=[pl.BlockSpec(memory_space=pltpu.VMEM)] * 3,
            out_specs=[pl.BlockSpec(memory_space=pltpu.VMEM)] * 3,
            name="finish",
        )(*outs)
        return alpha.reshape(n_tasks), ga.T, gb

    return jax.shard_map(device_step, mesh=mesh, in_specs=(P("data", None), P(None, "data"), P(), P(), P(), P(), P()), out_specs=(P(), P("data", None), P(None, "data")), check_vma=False)
```

```python
import functools

import jax
import jax.numpy as jnp
from jax import lax
from jax.experimental import pallas as pl
from jax.experimental.pallas import tpu as pltpu
from jax.sharding import PartitionSpec as P

EG_STEPS = 20
BF = jnp.bfloat16
F32 = jnp.float32
GELU_C = 0.7978845608028654
GELU_A = 0.044715
MESH = pl.DeviceIdType.MESH
BITS = (1, 2, 4, 8)
STRIP = 32
NT = (((1,), (1,)), ((), ()))
TN = (((0,), (0,)), ((), ()))


def xor(a, b):
    return sum(bit * ((a // bit + b // bit) % 2) for bit in BITS)


def mm(a, b, dims=(((1,), (0,)), ((), ()))):
    return lax.dot_general(a, b, dims, preferred_element_type=F32)


def kernel(cfg, x_hbm, lab_hbm, w1_hbm, w2_hbm, a_hbm, b_hbm, head_hbm, alpha_ref, ga_ref, gb_ref, xu, w1b, w2, a_v, head_v, lab_v, head_t, u_t, act, slope, z, dz, dp0, dp1, du_t, send_b, recv_b, send_a, recv_a, send_m, recv_m, load_sem, sb_sem, rb_sem, sa_sem, ra_sem, sm_sem, rm_sem):
    n_dev, total = cfg
    tok, d_model = x_hbm.shape
    d_ff = w1_hbm.shape[1]
    rank = a_hbm.shape[0]
    n_cls, n_task = head_hbm.shape[0], head_hbm.shape[1]
    col = d_ff // n_dev
    fc = 2 * col
    n_ch = n_dev // 2
    me = lax.axis_index("data")
    chip, core = me // 2, me % 2

    barrier = pltpu.get_barrier_semaphore()
    for k in range(1, n_dev):
        pl.semaphore_signal(barrier, inc=1, device_id=(xor(me, k),), device_id_type=MESH)

    sem_at = [0]

    def load(src, dst):
        copy = pltpu.make_async_copy(src, dst, load_sem.at[sem_at[0]])
        sem_at[0] += 1
        copy.start()
        return copy

    load_h = load(head_hbm, head_v)
    load_a = load(a_hbm, a_v)
    load_x = load(x_hbm, xu.at[:, pl.ds(0, d_model)])
    load_b = load(b_hbm, w1b.at[pl.ds(d_model, rank), :])
    load_w1 = [load(w1_hbm.at[:, pl.ds(i * fc, fc)], w1b.at[pl.ds(0, d_model), pl.ds(i * fc, fc)]) for i in range(n_ch)]
    load_l = load(lab_hbm, lab_v)
    w2_rows = d_ff // 4
    load_w2 = [load(w2_hbm.at[pl.ds(i * w2_rows, w2_rows), :], w2.at[pl.ds(i * w2_rows, w2_rows), :]) for i in range(4)]

    pad = xu.shape[1] - d_model
    xu[:, d_model:] = jnp.zeros((tok, pad), BF)
    w1b[d_model + rank:, :] = jnp.zeros((pad - rank, d_ff), BF)
    head_t[...] = jnp.zeros_like(head_t)
    load_h.wait()
    for t in range(n_task):
        head_t[32 * t:32 * t + n_cls, :] = head_v[:, t, :]
    load_a.wait()
    load_b.wait()
    load_x.wait()
    low = mm(xu[:, :d_model], a_v[...], NT)
    xu[:, d_model:d_model + rank] = low.astype(BF)
    u_t[...] = low.T.astype(BF)

    def pre(i):
        slope[i] = mm(xu[...], w1b[:, i * fc:i * fc + fc])

    def gelu(i):
        cols = slice(i * fc, i * fc + fc)
        for r in range(0, tok, STRIP):
            rs = slice(r, r + STRIP)
            x = slope[i, rs, :]
            x2 = x * x
            t = jnp.tanh(x * (GELU_C + (GELU_C * GELU_A) * x2))
            t1 = 1.0 + t
            g = (0.5 * x) * t1
            act[rs, cols] = g.astype(BF)
            slope[i, rs, :] = 0.5 * t1 + (g * (1.0 - t)) * (GELU_C + (3.0 * GELU_C * GELU_A) * x2)

    def stage(first, last):
        @pl.when(me >= 0)
        def _():
            for i in range(first, last):
                pre(i)
                if i:
                    gelu(i - 1)

    load_w1[0].wait()
    stage(0, 1)
    for w in load_w1[1:3]:
        w.wait()
    stage(1, 3)
    for w in load_w1[3:]:
        w.wait()
    stage(3, n_ch)
    for w in load_w2:
        w.wait()
    load_l.wait()
    hl = tok // 2
    zc = d_model // 2

    def out_block(h, n):
        cs = slice(n * zc, n * zc + zc)
        zz = mm(act[h * hl:h * hl + hl, :], w2[:, cs])
        for r in range(0, hl, STRIP):
            rs = slice(h * hl + r, h * hl + r + STRIP)
            z[rs, cs] = (xu[rs, cs].astype(F32) + zz[r:r + STRIP]).astype(BF)

    def errors(h):
        hs = slice(h * hl, h * hl + hl)
        logits = mm(head_t[...], z[hs, :], NT)
        rows = lax.broadcasted_iota(jnp.int32, (32, hl), 0)
        out = []
        for t in range(n_task):
            lg = jnp.where(rows < n_cls, logits[32 * t:32 * t + 32], -jnp.inf)
            ex = jnp.exp(lg - jnp.max(lg, axis=0, keepdims=True))
            prob = ex / jnp.sum(ex, axis=0, keepdims=True)
            out.append((prob - (rows == lab_v[t:t + 1, hs]).astype(F32)).astype(BF))
        return out

    def d_trunk(h, errs):
        for t in range(n_task):
            dz[tok * t + h * hl:tok * t + h * hl + hl, :] = mm(errs[t], head_t[32 * t:32 * t + 32, :], TN).astype(BF)

    @pl.when(me >= 0)
    def _():
        gelu(n_ch - 1)
        out_block(0, 0)
        out_block(0, 1)
        out_block(1, 0)
        errs0 = errors(0)
        out_block(1, 1)
        errs1 = errors(1)
        d_trunk(0, errs0)
        d_trunk(1, errs1)

    pl.semaphore_wait(barrier, n_dev - 1)

    def chunk_of(kk):
        return xor(chip, kk)

    def b_copy(t, kk, half):
        k = 2 * kk + (core + half) % 2
        return pltpu.make_async_remote_copy(
            src_ref=send_b.at[t, kk, half], dst_ref=recv_b.at[t, k - 1], send_sem=sb_sem.at[t], recv_sem=rb_sem.at[t],
            device_id=(2 * chunk_of(kk) + half,), device_id_type=MESH)

    def a_copy(t, k):
        dst = xor(me, k)
        return pltpu.make_async_remote_copy(
            src_ref=send_a.at[t, dst], dst_ref=recv_a.at[t, k - 1], send_sem=sa_sem.at[t], recv_sem=ra_sem.at[t],
            device_id=(dst,), device_id_type=MESH)

    def m_copy(k):
        return pltpu.make_async_remote_copy(
            src_ref=send_m, dst_ref=recv_m.at[k - 1], send_sem=sm_sem.at[0], recv_sem=rm_sem.at[0],
            device_id=(xor(me, k),), device_id_type=MESH)

    order = [15, 14, 13, 11, 10, 7, 6, 12, 9, 5, 3, 8, 4, 2, 1]
    lane8 = lax.broadcasted_iota(jnp.int32, (8, 128), 1)

    def wait_all(ref, sem):
        pltpu.make_async_copy(ref, ref, sem).wait()

    def d_pre(t, kk, dp_ref):
        c = chunk_of(kk)
        dh = mm(dz[pl.ds(pl.multiple_of(t * tok, tok), tok), :], w2[pl.ds(pl.multiple_of(c * fc, fc), fc), :], NT)
        dp_ref[...] = (dh * slope[c]).astype(BF)

    def grads(t, kk, dp_ref):
        c = chunk_of(kk)
        bm = w1b[pl.ds(d_model, rank), pl.ds(pl.multiple_of(c * fc, fc), fc)]
        part = mm(bm, dp_ref[...], NT)
        du_t[...] = part if kk == n_ch - 1 else du_t[...] + part
        gb = mm(u_t[...], dp_ref[...])
        for half in range(2):
            send_b[t, kk, half] = gb[:, col * half:col * half + col]

    def low_grad(t):
        ga = mm(du_t[...].astype(BF), xu[:, :d_model])
        for j in range(n_ch):
            top, low = ga[0:8, 128 * j:128 * j + 128], ga[8:16, 128 * j:128 * j + 128]
            send_a[t, 2 * j] = jnp.where(lane8 < 64, top, pltpu.roll(low, 64, 1))
            send_a[t, 2 * j + 1] = jnp.where(lane8 < 64, pltpu.roll(top, 64, 1), low)
        for k in order:
            a_copy(t, k).start()

    groups = {4: (7, 6, 5, 4), 2: (3, 2)}

    def task(t, _):
        dps = (dp0, dp1)
        d_pre(t, n_ch - 1, dps[1])
        for kk in reversed(range(n_ch)):
            if kk:
                d_pre(t, kk - 1, dps[(kk - 1) % 2])
            grads(t, kk, dps[kk % 2])
            for k2 in groups.get(kk, ()):
                b_copy(t, k2, 0).start()
                b_copy(t, k2, 1).start()
        low_grad(t)
        b_copy(t, 1, 0).start()
        b_copy(t, 1, 1).start()
        b_copy(t, 0, 1 - core).start()
        return 0

    lax.fori_loop(0, n_task, task, 0)

    inv = 1.0 / total

    def sum_up(own, recv, sem):
        wait_all(recv, sem)
        s = own
        for k in range(n_dev - 1):
            s = s + recv[k]
        return s * inv

    b_sum = [sum_up(send_b[t, 0, core], recv_b.at[t], rb_sem.at[t]) for t in range(n_task)]
    a_sum = [sum_up(send_a[t, me], recv_a.at[t], ra_sem.at[t]) for t in range(n_task)]

    def fold(part_b, part_a):
        return jnp.sum(part_b[:8, :128] + part_b[:8, 128:] + part_b[8:, :128] + part_b[8:, 128:] + part_a, axis=0, keepdims=True)

    b0, b1 = b_sum
    a0, a1 = a_sum
    s0 = fold(b0 * b0, a0 * a0)
    s1 = fold(b1 * b1, a1 * a1)
    mix = fold(b0 * b1, a0 * a1)
    send_m[0:1, :] = s0 - s1
    send_m[1:2, :] = s0 + s1
    send_m[2:3, :] = mix
    send_m[3:4, :] = jnp.zeros_like(mix)
    for k in order:
        m_copy(k).start()
    sum_m = send_m[...]
    wait_all(recv_m, rm_sem.at[0])
    for k in range(n_dev - 1):
        sum_m = sum_m + recv_m[k]
    gram = jnp.broadcast_to(jnp.sum(sum_m, axis=1, keepdims=True), sum_m.shape)
    m_diff, m_both, m_mix = gram[0:1], gram[1:2], gram[2:3]
    scale = 0.5 / m_both
    c0 = m_diff * scale
    c1 = (m_both - 2.0 * m_mix) * scale
    e = jnp.zeros_like(c0)
    for _ in range(EG_STEPS):
        e = (e - c0) - c1 * jnp.tanh(e)
    al0 = 1.0 / (1.0 + jnp.exp(-2.0 * e))
    al1 = 1.0 / (1.0 + jnp.exp(2.0 * e))
    gb_ref[...] = al0[:, 0:1] * b0 + al1[:, 0:1] * b1
    comb = al0 * a0 + al1 * a1
    ga_ref[0:8, :] = comb[:, :64]
    ga_ref[8:16, :] = pltpu.roll(comb, 64, 1)[:, :64]
    alpha_ref[...] = jnp.where(lane8[0:1, :] == 0, al0, al1)[:, 0:2]
    for t in range(n_task):
        wait_all(recv_b.at[t], sb_sem.at[t])
        wait_all(recv_a.at[t], sa_sem.at[t])
    wait_all(recv_m, sm_sem.at[0])


def finish(alpha_in, ga_in, gb_in, alpha_ref, ga_ref, gb_ref):
    alpha_ref[...] = alpha_in[...]
    ga_ref[...] = ga_in[...]
    gb_ref[...] = gb_in[...]


def solution(mesh):
    n_dev = mesh.shape["data"]

    def device_step(tokens, labels, w_one, w_two, adapter_a, adapter_b, task_heads):
        tok, d_model = tokens.shape
        d_ff = w_one.shape[1]
        rank = adapter_a.shape[1]
        n_tasks, _, n_cls = task_heads.shape
        col = d_ff // n_dev
        fc = 2 * col
        dma = pltpu.SemaphoreType.DMA
        outs = pl.pallas_call(
            functools.partial(kernel, (n_dev, tok * n_dev)),
            out_shape=(
                pltpu.VMEM((1, n_tasks), F32),
                pltpu.VMEM((rank, d_model // n_dev), F32),
                pltpu.VMEM((rank, col), F32),
            ),
            in_specs=[pl.BlockSpec(memory_space=pl.ANY)] * 7,
            out_specs=[pl.BlockSpec(memory_space=pltpu.VMEM)] * 3,
            scratch_shapes=[
                pltpu.VMEM((tok, d_model + 128), BF),
                pltpu.VMEM((d_model + 128, d_ff), BF),
                pltpu.VMEM((d_ff, d_model), BF),
                pltpu.VMEM((rank, d_model), BF),
                pltpu.VMEM((n_cls, n_tasks, d_model), BF),
                pltpu.VMEM((n_tasks, tok), jnp.int32),
                pltpu.VMEM((n_tasks * 32, d_model), BF),
                pltpu.VMEM((rank, tok), BF),
                pltpu.VMEM((tok, d_ff), BF),
                pltpu.VMEM((n_dev // 2, tok, fc), F32),
                pltpu.VMEM((tok, d_model), BF),
                pltpu.VMEM((n_tasks * tok, d_model), BF),
                pltpu.VMEM((tok, fc), BF),
                pltpu.VMEM((tok, fc), BF),
                pltpu.VMEM((rank, tok), F32),
                pltpu.VMEM((n_tasks, n_dev // 2, 2, rank, col), F32),
                pltpu.VMEM((n_tasks, n_dev - 1, rank, col), F32),
                pltpu.VMEM((n_tasks, n_dev, 8, 128), F32),
                pltpu.VMEM((n_tasks, n_dev - 1, 8, 128), F32),
                pltpu.VMEM((4, 128), F32),
                pltpu.VMEM((n_dev - 1, 4, 128), F32),
                dma((n_dev // 2 + 9,)),
                dma((n_tasks,)), dma((n_tasks,)), dma((n_tasks,)), dma((n_tasks,)), dma((1,)), dma((1,)),
            ],
            compiler_params=pltpu.CompilerParams(collective_id=0, has_side_effects=True, vmem_limit_bytes=60 * 1024 * 1024),
            name="step",
        )(tokens, labels, w_one, w_two, adapter_a.T, adapter_b, task_heads.transpose(2, 0, 1))
        alpha, ga, gb = pl.pallas_call(
            finish,
            out_shape=[jax.ShapeDtypeStruct(o.shape, o.dtype) for o in outs],
            in_specs=[pl.BlockSpec(memory_space=pltpu.VMEM)] * 3,
            out_specs=[pl.BlockSpec(memory_space=pltpu.VMEM)] * 3,
            name="finish",
        )(*[pltpu.with_memory_space_constraint(o, pltpu.VMEM) for o in outs])
        return alpha.reshape(n_tasks), ga.T, gb

    return jax.shard_map(device_step, mesh=mesh, in_specs=(P("data", None), P(None, "data"), P(), P(), P(), P(), P()), out_specs=(P(), P("data", None), P(None, "data")), check_vma=False)
```

```python
import functools

import jax
import jax.numpy as jnp
from jax import lax
from jax.experimental import pallas as pl
from jax.experimental.pallas import tpu as pltpu
from jax.sharding import PartitionSpec as P

EG_STEPS = 20
BF = jnp.bfloat16
F32 = jnp.float32
GELU_C = 0.7978845608028654
GELU_A = 0.044715
MESH = pl.DeviceIdType.MESH
BITS = (1, 2, 4, 8)
STRIP = 32
NT = (((1,), (1,)), ((), ()))
TN = (((0,), (0,)), ((), ()))


def xor(a, b):
    return sum(bit * ((a // bit + b // bit) % 2) for bit in BITS)


def mm(a, b, dims=(((1,), (0,)), ((), ()))):
    return lax.dot_general(a, b, dims, preferred_element_type=F32)


def kernel(cfg, x_hbm, lab_hbm, w1_hbm, w2_hbm, a_hbm, b_hbm, head_hbm, alpha_ref, ga_ref, gb_ref, xu, w1b, w2, a_v, head_v, lab_v, head_t, u_t, act, slope, z, dz, dp0, dp1, dpt0, dpt1, du_t, send_b, recv_b, send_a, recv_a, send_m, recv_m, load_sem, sb_sem, rb_sem, sa_sem, ra_sem, sm_sem, rm_sem):
    n_dev, total = cfg
    tok, d_model = x_hbm.shape
    d_ff = w1_hbm.shape[1]
    rank = a_hbm.shape[0]
    n_cls, n_task = head_hbm.shape[0], head_hbm.shape[1]
    col = d_ff // n_dev
    fc = 2 * col
    n_ch = n_dev // 2
    me = lax.axis_index("data")
    chip, core = me // 2, me % 2

    barrier = pltpu.get_barrier_semaphore()
    for k in range(1, n_dev):
        pl.semaphore_signal(barrier, inc=1, device_id=(xor(me, k),), device_id_type=MESH)

    sem_at = [0]

    def load(src, dst):
        copy = pltpu.make_async_copy(src, dst, load_sem.at[sem_at[0]])
        sem_at[0] += 1
        copy.start()
        return copy

    load_h = load(head_hbm, head_v)
    load_a = load(a_hbm, a_v)
    load_x = load(x_hbm, xu.at[:, pl.ds(0, d_model)])
    load_b = load(b_hbm, w1b.at[pl.ds(d_model, rank), :])
    load_w1 = [load(w1_hbm.at[:, pl.ds(i * fc, fc)], w1b.at[pl.ds(0, d_model), pl.ds(i * fc, fc)]) for i in range(n_ch)]
    load_l = load(lab_hbm, lab_v)
    w2_rows = d_ff // 4
    load_w2 = [load(w2_hbm.at[pl.ds(i * w2_rows, w2_rows), :], w2.at[pl.ds(i * w2_rows, w2_rows), :]) for i in range(4)]

    pad = xu.shape[1] - d_model
    xu[:, d_model:] = jnp.zeros((tok, pad), BF)
    w1b[d_model + rank:, :] = jnp.zeros((pad - rank, d_ff), BF)
    head_t[...] = jnp.zeros_like(head_t)
    load_h.wait()
    for t in range(n_task):
        head_t[32 * t:32 * t + n_cls, :] = head_v[:, t, :]
    load_a.wait()
    load_b.wait()
    load_x.wait()
    low = mm(xu[:, :d_model], a_v[...], NT)
    xu[:, d_model:d_model + rank] = low.astype(BF)
    u_t[...] = low.T.astype(BF)

    def pre(i):
        slope[i] = mm(xu[...], w1b[:, i * fc:i * fc + fc])

    def gelu(i):
        cols = slice(i * fc, i * fc + fc)
        for r in range(0, tok, STRIP):
            rs = slice(r, r + STRIP)
            x = slope[i, rs, :]
            x2 = x * x
            t = jnp.tanh(x * (GELU_C + (GELU_C * GELU_A) * x2))
            t1 = 1.0 + t
            g = (0.5 * x) * t1
            act[rs, cols] = g.astype(BF)
            slope[i, rs, :] = 0.5 * t1 + (g * (1.0 - t)) * (GELU_C + (3.0 * GELU_C * GELU_A) * x2)

    def stage(first, last):
        @pl.when(me >= 0)
        def _():
            for i in range(first, last):
                pre(i)
                if i:
                    gelu(i - 1)

    load_w1[0].wait()
    stage(0, 1)
    for w in load_w1[1:3]:
        w.wait()
    stage(1, 3)
    for w in load_w1[3:]:
        w.wait()
    stage(3, n_ch)
    for w in load_w2:
        w.wait()
    load_l.wait()
    hl = tok // 2
    zc = d_model // 2

    def out_block(h, n):
        cs = slice(n * zc, n * zc + zc)
        zz = mm(act[h * hl:h * hl + hl, :], w2[:, cs])
        for r in range(0, hl, STRIP):
            rs = slice(h * hl + r, h * hl + r + STRIP)
            z[rs, cs] = (xu[rs, cs].astype(F32) + zz[r:r + STRIP]).astype(BF)

    def errors(h):
        hs = slice(h * hl, h * hl + hl)
        logits = mm(head_t[...], z[hs, :], NT)
        rows = lax.broadcasted_iota(jnp.int32, (32, hl), 0)
        out = []
        for t in range(n_task):
            lg = jnp.where(rows < n_cls, logits[32 * t:32 * t + 32], -jnp.inf)
            ex = jnp.exp(lg - jnp.max(lg, axis=0, keepdims=True))
            prob = ex / jnp.sum(ex, axis=0, keepdims=True)
            out.append((prob - (rows == lab_v[t:t + 1, hs]).astype(F32)).astype(BF))
        return out

    def d_trunk(h, errs):
        for t in range(n_task):
            dz[tok * t + h * hl:tok * t + h * hl + hl, :] = mm(errs[t], head_t[32 * t:32 * t + 32, :], TN).astype(BF)

    @pl.when(me >= 0)
    def _():
        gelu(n_ch - 1)
        out_block(0, 0)
        out_block(0, 1)
        out_block(1, 0)
        errs0 = errors(0)
        out_block(1, 1)
        errs1 = errors(1)
        d_trunk(0, errs0)
        d_trunk(1, errs1)

    pl.semaphore_wait(barrier, n_dev - 1)

    def chunk_of(kk):
        return xor(chip, kk)

    def b_copy(t, kk, half):
        k = 2 * kk + (core + half) % 2
        return pltpu.make_async_remote_copy(
            src_ref=send_b.at[t, kk, half], dst_ref=recv_b.at[t, k - 1], send_sem=sb_sem.at[t], recv_sem=rb_sem.at[t],
            device_id=(2 * chunk_of(kk) + half,), device_id_type=MESH)

    def a_copy(t, k):
        dst = xor(me, k)
        return pltpu.make_async_remote_copy(
            src_ref=send_a.at[t, dst], dst_ref=recv_a.at[t, k - 1], send_sem=sa_sem.at[t], recv_sem=ra_sem.at[t],
            device_id=(dst,), device_id_type=MESH)

    def m_copy(k):
        return pltpu.make_async_remote_copy(
            src_ref=send_m, dst_ref=recv_m.at[k - 1], send_sem=sm_sem.at[0], recv_sem=rm_sem.at[0],
            device_id=(xor(me, k),), device_id_type=MESH)

    order = [15, 14, 13, 11, 10, 7, 6, 12, 9, 5, 3, 8, 4, 2, 1]
    lane8 = lax.broadcasted_iota(jnp.int32, (8, 128), 1)

    def wait_all(ref, sem):
        pltpu.make_async_copy(ref, ref, sem).wait()

    def d_pre(t, kk, dp_ref, dpt_ref):
        c = chunk_of(kk)
        dh = mm(dz[tok * t:tok * t + tok, :], w2[pl.ds(pl.multiple_of(c * fc, fc), fc), :], NT)
        dp = (dh * slope[c]).astype(BF)
        dp_ref[...] = dp
        dpt_ref[...] = dp.T

    def grads(t, kk, dp_ref, dpt_ref):
        c = chunk_of(kk)
        bm = w1b[pl.ds(d_model, rank), pl.ds(pl.multiple_of(c * fc, fc), fc)]
        part = mm(bm, dpt_ref[...])
        du_t[t] = part if kk == n_ch - 1 else du_t[t] + part
        gb = mm(u_t[...], dp_ref[...])
        for half in range(2):
            send_b[t, kk, half] = gb[:, col * half:col * half + col]

    def low_grad(t):
        ga = mm(du_t[t].astype(BF), xu[:, :d_model])
        for j in range(n_ch):
            top, low = ga[0:8, 128 * j:128 * j + 128], ga[8:16, 128 * j:128 * j + 128]
            send_a[t, 2 * j] = jnp.where(lane8 < 64, top, pltpu.roll(low, 64, 1))
            send_a[t, 2 * j + 1] = jnp.where(lane8 < 64, pltpu.roll(top, 64, 1), low)
        for k in order:
            a_copy(t, k).start()

    def send_group(t, group):
        for kk in group:
            if kk:
                b_copy(t, kk, 0).start()
                b_copy(t, kk, 1).start()
            else:
                b_copy(t, 0, 1 - core).start()

    units = [(t, kk) for t in range(n_task) for kk in reversed(range(n_ch))]
    dps = (dp0, dp1)
    dpts = (dpt0, dpt1)
    d_pre(*units[0], dps[0], dpts[0])
    for j, (t, kk) in enumerate(units):
        if j + 1 < len(units):
            d_pre(*units[j + 1], dps[(j + 1) % 2], dpts[(j + 1) % 2])
        grads(t, kk, dps[j % 2], dpts[j % 2])
        if kk == 4:
            send_group(t, (7, 6, 5, 4))
        if kk == 2 and t == n_task - 1:
            send_group(t, (3, 2))
        if kk == 0:
            low_grad(t)
            send_group(t, (1, 0) if t == n_task - 1 else (3, 2, 1, 0))

    inv = 1.0 / total

    def sum_up(own, recv, sem):
        wait_all(recv, sem)
        s = own
        for k in range(n_dev - 1):
            s = s + recv[k]
        return s * inv

    b_sum = [sum_up(send_b[t, 0, core], recv_b.at[t], rb_sem.at[t]) for t in range(n_task)]
    a_sum = [sum_up(send_a[t, me], recv_a.at[t], ra_sem.at[t]) for t in range(n_task)]

    def fold(part_b, part_a):
        return jnp.sum(part_b[:8, :128] + part_b[:8, 128:] + part_b[8:, :128] + part_b[8:, 128:] + part_a, axis=0, keepdims=True)

    b0, b1 = b_sum
    a0, a1 = a_sum
    s0 = fold(b0 * b0, a0 * a0)
    s1 = fold(b1 * b1, a1 * a1)
    mix = fold(b0 * b1, a0 * a1)
    send_m[0:1, :] = s0 - s1
    send_m[1:2, :] = s0 + s1
    send_m[2:3, :] = mix
    send_m[3:4, :] = jnp.zeros_like(mix)
    for k in order:
        m_copy(k).start()
    sum_m = send_m[...]
    wait_all(recv_m, rm_sem.at[0])
    for k in range(n_dev - 1):
        sum_m = sum_m + recv_m[k]
    gram = jnp.broadcast_to(jnp.sum(sum_m, axis=1, keepdims=True), sum_m.shape)
    m_diff, m_both, m_mix = gram[0:1], gram[1:2], gram[2:3]
    scale = 0.5 / m_both
    c0 = m_diff * scale
    c1 = (m_both - 2.0 * m_mix) * scale
    e = jnp.zeros_like(c0)
    for _ in range(EG_STEPS):
        e = (e - c0) - c1 * jnp.tanh(e)
    al0 = 1.0 / (1.0 + jnp.exp(-2.0 * e))
    al1 = 1.0 / (1.0 + jnp.exp(2.0 * e))
    gb_ref[...] = al0[:, 0:1] * b0 + al1[:, 0:1] * b1
    comb = al0 * a0 + al1 * a1
    ga_ref[0:8, :] = comb[:, :64]
    ga_ref[8:16, :] = pltpu.roll(comb, 64, 1)[:, :64]
    alpha_ref[...] = jnp.where(lane8[0:1, :] == 0, al0, al1)[:, 0:2]
    for t in range(n_task):
        wait_all(recv_b.at[t], sb_sem.at[t])
        wait_all(recv_a.at[t], sa_sem.at[t])
    wait_all(recv_m, sm_sem.at[0])


def finish(alpha_in, ga_in, gb_in, alpha_ref, ga_ref, gb_ref):
    alpha_ref[...] = alpha_in[...]
    ga_ref[...] = ga_in[...]
    gb_ref[...] = gb_in[...]


def solution(mesh):
    n_dev = mesh.shape["data"]

    def device_step(tokens, labels, w_one, w_two, adapter_a, adapter_b, task_heads):
        tok, d_model = tokens.shape
        d_ff = w_one.shape[1]
        rank = adapter_a.shape[1]
        n_tasks, _, n_cls = task_heads.shape
        col = d_ff // n_dev
        fc = 2 * col
        dma = pltpu.SemaphoreType.DMA
        outs = pl.pallas_call(
            functools.partial(kernel, (n_dev, tok * n_dev)),
            out_shape=(
                pltpu.VMEM((1, n_tasks), F32),
                pltpu.VMEM((rank, d_model // n_dev), F32),
                pltpu.VMEM((rank, col), F32),
            ),
            in_specs=[pl.BlockSpec(memory_space=pl.ANY)] * 7,
            out_specs=[pl.BlockSpec(memory_space=pltpu.VMEM)] * 3,
            scratch_shapes=[
                pltpu.VMEM((tok, d_model + 128), BF),
                pltpu.VMEM((d_model + 128, d_ff), BF),
                pltpu.VMEM((d_ff, d_model), BF),
                pltpu.VMEM((rank, d_model), BF),
                pltpu.VMEM((n_cls, n_tasks, d_model), BF),
                pltpu.VMEM((n_tasks, tok), jnp.int32),
                pltpu.VMEM((n_tasks * 32, d_model), BF),
                pltpu.VMEM((rank, tok), BF),
                pltpu.VMEM((tok, d_ff), BF),
                pltpu.VMEM((n_dev // 2, tok, fc), F32),
                pltpu.VMEM((tok, d_model), BF),
                pltpu.VMEM((n_tasks * tok, d_model), BF),
                pltpu.VMEM((tok, fc), BF),
                pltpu.VMEM((tok, fc), BF),
                pltpu.VMEM((fc, tok), BF),
                pltpu.VMEM((fc, tok), BF),
                pltpu.VMEM((n_tasks, rank, tok), F32),
                pltpu.VMEM((n_tasks, n_dev // 2, 2, rank, col), F32),
                pltpu.VMEM((n_tasks, n_dev - 1, rank, col), F32),
                pltpu.VMEM((n_tasks, n_dev, 8, 128), F32),
                pltpu.VMEM((n_tasks, n_dev - 1, 8, 128), F32),
                pltpu.VMEM((4, 128), F32),
                pltpu.VMEM((n_dev - 1, 4, 128), F32),
                dma((n_dev // 2 + 9,)),
                dma((n_tasks,)), dma((n_tasks,)), dma((n_tasks,)), dma((n_tasks,)), dma((1,)), dma((1,)),
            ],
            compiler_params=pltpu.CompilerParams(collective_id=0, has_side_effects=True, vmem_limit_bytes=60 * 1024 * 1024),
            name="step",
        )(tokens, labels, w_one, w_two, adapter_a.T, adapter_b, task_heads.transpose(2, 0, 1))
        alpha, ga, gb = pl.pallas_call(
            finish,
            out_shape=[jax.ShapeDtypeStruct(o.shape, o.dtype) for o in outs],
            in_specs=[pl.BlockSpec(memory_space=pltpu.VMEM)] * 3,
            out_specs=[pl.BlockSpec(memory_space=pltpu.VMEM)] * 3,
            name="finish",
        )(*[pltpu.with_memory_space_constraint(o, pltpu.VMEM) for o in outs])
        return alpha.reshape(n_tasks), ga.T, gb

    return jax.shard_map(device_step, mesh=mesh, in_specs=(P("data", None), P(None, "data"), P(), P(), P(), P(), P()), out_specs=(P(), P("data", None), P(None, "data")), check_vma=False)
```

```python
import functools

import jax
import jax.numpy as jnp
from jax import lax
from jax.experimental import pallas as pl
from jax.experimental.pallas import tpu as pltpu
from jax.sharding import PartitionSpec as P

EG_STEPS = 20
BF = jnp.bfloat16
F32 = jnp.float32
GELU_C = 0.7978845608028654
GELU_A = 0.044715
MESH = pl.DeviceIdType.MESH
BITS = (1, 2, 4, 8)
STRIP = 16
NT = (((1,), (1,)), ((), ()))
TN = (((0,), (0,)), ((), ()))


def xor(a, b):
    return sum(bit * ((a // bit + b // bit) % 2) for bit in BITS)


def mm(a, b, dims=(((1,), (0,)), ((), ()))):
    return lax.dot_general(a, b, dims, preferred_element_type=F32)


def kernel(cfg, x_hbm, lab_hbm, w1_hbm, w2_hbm, a_hbm, b_hbm, head_hbm, alpha_ref, ga_ref, gb_ref, xu, w1b, w2, a_v, head_v, lab_v, head_t, u_t, act, slope, z, dz, dp0, dp1, dpt0, dpt1, du_t, send_b, recv_b, send_a, recv_a, send_m, recv_m, load_sem, sb_sem, rb_sem, sa_sem, ra_sem, sm_sem, rm_sem):
    n_dev, total = cfg
    tok, d_model = x_hbm.shape
    d_ff = w1_hbm.shape[1]
    rank = a_hbm.shape[0]
    n_cls, n_task = head_hbm.shape[0], head_hbm.shape[1]
    col = d_ff // n_dev
    fc = 2 * col
    n_ch = n_dev // 2
    me = lax.axis_index("data")
    chip, core = me // 2, me % 2

    barrier = pltpu.get_barrier_semaphore()
    for k in range(1, n_dev):
        pl.semaphore_signal(barrier, inc=1, device_id=(xor(me, k),), device_id_type=MESH)

    sem_at = [0]

    def load(src, dst):
        copy = pltpu.make_async_copy(src, dst, load_sem.at[sem_at[0]])
        sem_at[0] += 1
        copy.start()
        return copy

    load_h = load(head_hbm, head_v)
    load_a = load(a_hbm, a_v)
    load_x = load(x_hbm, xu.at[:, pl.ds(0, d_model)])
    load_b = load(b_hbm, w1b.at[pl.ds(d_model, rank), :])
    load_w1 = [load(w1_hbm.at[:, pl.ds(i * fc, fc)], w1b.at[pl.ds(0, d_model), pl.ds(i * fc, fc)]) for i in range(n_ch)]
    load_l = load(lab_hbm, lab_v)
    w2_rows = d_ff // 4
    load_w2 = [load(w2_hbm.at[pl.ds(i * w2_rows, w2_rows), :], w2.at[pl.ds(i * w2_rows, w2_rows), :]) for i in range(4)]

    pad = xu.shape[1] - d_model
    xu[:, d_model:] = jnp.zeros((tok, pad), BF)
    w1b[d_model + rank:, :] = jnp.zeros((pad - rank, d_ff), BF)
    head_t[...] = jnp.zeros_like(head_t)
    load_h.wait()
    for t in range(n_task):
        head_t[32 * t:32 * t + n_cls, :] = head_v[:, t, :]
    load_a.wait()
    load_b.wait()
    load_x.wait()
    low = mm(xu[:, :d_model], a_v[...], NT)
    xu[:, d_model:d_model + rank] = low.astype(BF)
    u_t[...] = low.T.astype(BF)

    def pre(i):
        slope[i] = mm(xu[...], w1b[:, i * fc:i * fc + fc])

    def gelu(i):
        cols = slice(i * fc, i * fc + fc)
        for r in range(0, tok, STRIP):
            rs = slice(r, r + STRIP)
            x = slope[i, rs, :]
            x2 = x * x
            t = jnp.tanh(x * (GELU_C + (GELU_C * GELU_A) * x2))
            t1 = 1.0 + t
            g = (0.5 * x) * t1
            act[rs, cols] = g.astype(BF)
            slope[i, rs, :] = 0.5 * t1 + (g * (1.0 - t)) * (GELU_C + (3.0 * GELU_C * GELU_A) * x2)

    def stage(first, last):
        @pl.when(me >= 0)
        def _():
            for i in range(first, last):
                pre(i)
                if i:
                    gelu(i - 1)

    load_w1[0].wait()
    stage(0, 1)
    for w in load_w1[1:3]:
        w.wait()
    stage(1, 3)
    for w in load_w1[3:]:
        w.wait()
    stage(3, n_ch)
    for w in load_w2:
        w.wait()
    load_l.wait()
    hl = tok // 2
    zc = d_model // 2

    def out_block(h, n):
        cs = slice(n * zc, n * zc + zc)
        zz = mm(act[h * hl:h * hl + hl, :], w2[:, cs])
        for r in range(0, hl, STRIP):
            rs = slice(h * hl + r, h * hl + r + STRIP)
            z[rs, cs] = (xu[rs, cs].astype(F32) + zz[r:r + STRIP]).astype(BF)

    def errors(h):
        hs = slice(h * hl, h * hl + hl)
        logits = mm(head_t[...], z[hs, :], NT)
        rows = lax.broadcasted_iota(jnp.int32, (32, hl), 0)
        out = []
        for t in range(n_task):
            lg = jnp.where(rows < n_cls, logits[32 * t:32 * t + 32], -jnp.inf)
            ex = jnp.exp(lg - jnp.max(lg, axis=0, keepdims=True))
            prob = ex / jnp.sum(ex, axis=0, keepdims=True)
            out.append((prob - (rows == lab_v[t:t + 1, hs]).astype(F32)).astype(BF))
        return out

    def d_trunk(h, errs):
        for t in range(n_task):
            dz[tok * t + h * hl:tok * t + h * hl + hl, :] = mm(errs[t], head_t[32 * t:32 * t + 32, :], TN).astype(BF)

    @pl.when(me >= 0)
    def _():
        gelu(n_ch - 1)
        out_block(0, 0)
        out_block(0, 1)
        out_block(1, 0)
        errs0 = errors(0)
        out_block(1, 1)
        errs1 = errors(1)
        d_trunk(0, errs0)
        d_trunk(1, errs1)

    pl.semaphore_wait(barrier, n_dev - 1)

    def chunk_of(kk):
        return xor(chip, kk)

    def b_copy(t, kk, half):
        k = 2 * kk + (core + half) % 2
        return pltpu.make_async_remote_copy(
            src_ref=send_b.at[t, kk, half], dst_ref=recv_b.at[t, k - 1], send_sem=sb_sem.at[t], recv_sem=rb_sem.at[t],
            device_id=(2 * chunk_of(kk) + half,), device_id_type=MESH)

    def a_copy(t, k):
        dst = xor(me, k)
        return pltpu.make_async_remote_copy(
            src_ref=send_a.at[t, dst], dst_ref=recv_a.at[t, k - 1], send_sem=sa_sem.at[t], recv_sem=ra_sem.at[t],
            device_id=(dst,), device_id_type=MESH)

    def m_copy(k):
        return pltpu.make_async_remote_copy(
            src_ref=send_m, dst_ref=recv_m.at[k - 1], send_sem=sm_sem.at[0], recv_sem=rm_sem.at[0],
            device_id=(xor(me, k),), device_id_type=MESH)

    order = [15, 14, 13, 11, 10, 7, 6, 12, 9, 5, 3, 8, 4, 2, 1]
    lane8 = lax.broadcasted_iota(jnp.int32, (8, 128), 1)

    def wait_all(ref, sem):
        pltpu.make_async_copy(ref, ref, sem).wait()

    def d_pre(t, kk, dp_ref, dpt_ref):
        c = chunk_of(kk)
        dh = mm(dz[tok * t:tok * t + tok, :], w2[pl.ds(pl.multiple_of(c * fc, fc), fc), :], NT)
        dp = (dh * slope[c]).astype(BF)
        dp_ref[...] = dp
        dpt_ref[...] = dp.T

    def grads(t, kk, dp_ref, dpt_ref):
        c = chunk_of(kk)
        bm = w1b[pl.ds(d_model, rank), pl.ds(pl.multiple_of(c * fc, fc), fc)]
        part = mm(bm, dpt_ref[...])
        du_t[t] = part if kk == n_ch - 1 else du_t[t] + part
        gb = mm(u_t[...], dp_ref[...])
        for half in range(2):
            send_b[t, kk, half] = gb[:, col * half:col * half + col]

    def low_grad(t):
        ga = mm(du_t[t].astype(BF), xu[:, :d_model])
        for j in range(n_ch):
            top, low = ga[0:8, 128 * j:128 * j + 128], ga[8:16, 128 * j:128 * j + 128]
            send_a[t, 2 * j] = jnp.where(lane8 < 64, top, pltpu.roll(low, 64, 1))
            send_a[t, 2 * j + 1] = jnp.where(lane8 < 64, pltpu.roll(top, 64, 1), low)
        for k in order:
            a_copy(t, k).start()

    def send_group(t, group):
        for kk in group:
            if kk:
                b_copy(t, kk, 0).start()
                b_copy(t, kk, 1).start()
            else:
                b_copy(t, 0, 1 - core).start()

    units = [(t, kk) for t in range(n_task) for kk in reversed(range(n_ch))]
    dps = (dp0, dp1)
    dpts = (dpt0, dpt1)
    d_pre(*units[0], dps[0], dpts[0])
    for j, (t, kk) in enumerate(units):
        if j + 1 < len(units):
            d_pre(*units[j + 1], dps[(j + 1) % 2], dpts[(j + 1) % 2])
        grads(t, kk, dps[j % 2], dpts[j % 2])
        if kk == 4:
            send_group(t, (7, 6, 5, 4))
        if kk == 2 and t == n_task - 1:
            send_group(t, (3, 2))
        if kk == 0:
            low_grad(t)
            send_group(t, (1, 0) if t == n_task - 1 else (3, 2, 1, 0))

    inv = 1.0 / total

    def sum_up(own, recv, sem):
        wait_all(recv, sem)
        s = own
        for k in range(n_dev - 1):
            s = s + recv[k]
        return s * inv

    b_sum = [sum_up(send_b[t, 0, core], recv_b.at[t], rb_sem.at[t]) for t in range(n_task)]
    a_sum = [sum_up(send_a[t, me], recv_a.at[t], ra_sem.at[t]) for t in range(n_task)]

    def fold(part_b, part_a):
        return jnp.sum(part_b[:8, :128] + part_b[:8, 128:] + part_b[8:, :128] + part_b[8:, 128:] + part_a, axis=0, keepdims=True)

    b0, b1 = b_sum
    a0, a1 = a_sum
    s0 = fold(b0 * b0, a0 * a0)
    s1 = fold(b1 * b1, a1 * a1)
    mix = fold(b0 * b1, a0 * a1)
    send_m[0:1, :] = s0 - s1
    send_m[1:2, :] = s0 + s1
    send_m[2:3, :] = mix
    send_m[3:4, :] = jnp.zeros_like(mix)
    for k in order:
        m_copy(k).start()
    sum_m = send_m[...]
    wait_all(recv_m, rm_sem.at[0])
    for k in range(n_dev - 1):
        sum_m = sum_m + recv_m[k]
    gram = jnp.broadcast_to(jnp.sum(sum_m, axis=1, keepdims=True), sum_m.shape)
    m_diff, m_both, m_mix = gram[0:1], gram[1:2], gram[2:3]
    scale = 0.5 / m_both
    c0 = m_diff * scale
    c1 = (m_both - 2.0 * m_mix) * scale
    e = jnp.zeros_like(c0)
    for _ in range(EG_STEPS):
        e = (e - c0) - c1 * jnp.tanh(e)
    al0 = 1.0 / (1.0 + jnp.exp(-2.0 * e))
    al1 = 1.0 / (1.0 + jnp.exp(2.0 * e))
    gb_ref[...] = al0[:, 0:1] * b0 + al1[:, 0:1] * b1
    comb = al0 * a0 + al1 * a1
    ga_ref[0:8, :] = comb[:, :64]
    ga_ref[8:16, :] = pltpu.roll(comb, 64, 1)[:, :64]
    alpha_ref[...] = jnp.where(lane8[0:1, :] == 0, al0, al1)[:, 0:2]
    for t in range(n_task):
        wait_all(recv_b.at[t], sb_sem.at[t])
        wait_all(recv_a.at[t], sa_sem.at[t])
    wait_all(recv_m, sm_sem.at[0])


def finish(alpha_in, ga_in, gb_in, alpha_ref, ga_ref, gb_ref):
    alpha_ref[...] = alpha_in[...]
    ga_ref[...] = ga_in[...]
    gb_ref[...] = gb_in[...]


def solution(mesh):
    n_dev = mesh.shape["data"]

    def device_step(tokens, labels, w_one, w_two, adapter_a, adapter_b, task_heads):
        tok, d_model = tokens.shape
        d_ff = w_one.shape[1]
        rank = adapter_a.shape[1]
        n_tasks, _, n_cls = task_heads.shape
        col = d_ff // n_dev
        fc = 2 * col
        dma = pltpu.SemaphoreType.DMA
        outs = pl.pallas_call(
            functools.partial(kernel, (n_dev, tok * n_dev)),
            out_shape=(
                pltpu.VMEM((1, n_tasks), F32),
                pltpu.VMEM((rank, d_model // n_dev), F32),
                pltpu.VMEM((rank, col), F32),
            ),
            in_specs=[pl.BlockSpec(memory_space=pl.ANY)] * 7,
            out_specs=[pl.BlockSpec(memory_space=pltpu.VMEM)] * 3,
            scratch_shapes=[
                pltpu.VMEM((tok, d_model + 128), BF),
                pltpu.VMEM((d_model + 128, d_ff), BF),
                pltpu.VMEM((d_ff, d_model), BF),
                pltpu.VMEM((rank, d_model), BF),
                pltpu.VMEM((n_cls, n_tasks, d_model), BF),
                pltpu.VMEM((n_tasks, tok), jnp.int32),
                pltpu.VMEM((n_tasks * 32, d_model), BF),
                pltpu.VMEM((rank, tok), BF),
                pltpu.VMEM((tok, d_ff), BF),
                pltpu.VMEM((n_dev // 2, tok, fc), F32),
                pltpu.VMEM((tok, d_model), BF),
                pltpu.VMEM((n_tasks * tok, d_model), BF),
                pltpu.VMEM((tok, fc), BF),
                pltpu.VMEM((tok, fc), BF),
                pltpu.VMEM((fc, tok), BF),
                pltpu.VMEM((fc, tok), BF),
                pltpu.VMEM((n_tasks, rank, tok), F32),
                pltpu.VMEM((n_tasks, n_dev // 2, 2, rank, col), F32),
                pltpu.VMEM((n_tasks, n_dev - 1, rank, col), F32),
                pltpu.VMEM((n_tasks, n_dev, 8, 128), F32),
                pltpu.VMEM((n_tasks, n_dev - 1, 8, 128), F32),
                pltpu.VMEM((4, 128), F32),
                pltpu.VMEM((n_dev - 1, 4, 128), F32),
                dma((n_dev // 2 + 9,)),
                dma((n_tasks,)), dma((n_tasks,)), dma((n_tasks,)), dma((n_tasks,)), dma((1,)), dma((1,)),
            ],
            compiler_params=pltpu.CompilerParams(collective_id=0, has_side_effects=True, vmem_limit_bytes=60 * 1024 * 1024),
            name="step",
        )(tokens, labels, w_one, w_two, adapter_a.T, adapter_b, task_heads.transpose(2, 0, 1))
        alpha, ga, gb = pl.pallas_call(
            finish,
            out_shape=[jax.ShapeDtypeStruct(o.shape, o.dtype) for o in outs],
            in_specs=[pl.BlockSpec(memory_space=pltpu.VMEM)] * 3,
            out_specs=[pl.BlockSpec(memory_space=pltpu.VMEM)] * 3,
            name="finish",
        )(*[pltpu.with_memory_space_constraint(o, pltpu.VMEM) for o in outs])
        return alpha.reshape(n_tasks), ga.T, gb

    return jax.shard_map(device_step, mesh=mesh, in_specs=(P("data", None), P(None, "data"), P(), P(), P(), P(), P()), out_specs=(P(), P("data", None), P(None, "data")), check_vma=False)
```
